32 devices in a mesh: grp: 2 (over core), gx: 4 (over y, x), gy: 4 (over z).
Axes of the slice: x: 2, y: 2, z: 4, core: 2. Of those that a mesh axis runs over, the one named last changes fastest.
Arguments:
- coarse_density: float32 [512, 512, 512], P('gx', ('grp', 'gy')), may hold values from -3 to 3
- fine_density: float32 [32, 128, 256], P('gx', 'gy', 'grp'), may hold values from -96 to 96
- fine_start: float32 [32, 128, 256], P('gx', 'gy', 'grp'), may hold values from -6 to 6
- anchor: int32 [3], replicated, may hold values from 1 to 447
Outputs:
- coarse_potential: float32 [512, 512, 512], P('gx', ('grp', 'gy'))
- fine_potential: float32 [32, 128, 256], P('gx', 'gy', 'grp')
The draws below stay inside these ranges and needn't reach their ends.
Inputs may be any that keep to these rules, and one draw needn't show every extreme that they name: Along every dimension d the coarse cells anchor[d] - 1 up to anchor[d] + (fine cells along d) / 4 lie inside the coarse grid.
All inputs are finite; a program needn't handle non-finite values.
Results may differ from the reference program's by a relative error of at most 0.00015.
Values sent between devices are 32-bit elements; how exact they have to be, the bound alone decides.
A program may use at most 128 MiB of HBM per device.

```python
import math
import jax
import jax.numpy as jnp
from jax import lax

NC = 512
RATIO = 4
SWEEPS = 8
FX = 32
FY = 128
FZ = 256
CBX = 10
CBY = 34
CBZ = 66


def block_levels(rng, shape, pieces, low, high):
    def one(dim, parts):
        steps = jax.random.uniform(jax.random.fold_in(jax.random.fold_in(rng, 6), dim), (parts,), jnp.float32, low / len(pieces), high / len(pieces))
        return jnp.repeat(jnp.exp(steps), shape[dim] // parts).reshape((-1,) + (1,) * (len(shape) - dim - 1))

    factor_of = one(*pieces[0])
    for cut in pieces[1:]:
        factor_of = factor_of * one(*cut)
    return factor_of


def gaussian(key, extent, width, reach, cuts=(), kind=jnp.bfloat16):
    values = width * jax.random.normal(key, extent, jnp.float32)
    if cuts:
        values = values * block_levels(key, extent, cuts, -0.22, 0.18)
    return jnp.clip(values, -reach, reach).astype(kind)


def setup_inputs(seed: int = 0) -> dict:
    key_list = jax.random.split(jax.random.key(seed), 5)
    coarse_density = gaussian(key_list[0], (NC, NC, NC), 0.5, 3.0, ((0, 4), (1, 8)), jnp.float32)
    fine_density = gaussian(key_list[1], (FX, FY, FZ), 16.0, 96.0, ((0, 4), (1, 4), (2, 2)), jnp.float32)
    fine_start = gaussian(key_list[2], (FX, FY, FZ), 1.0, 6.0, ((0, 4), (1, 4), (2, 2)), jnp.float32)
    anchor = jax.random.randint(key_list[3], (3,), 1, NC - max(FX, max(FY, FZ)) // RATIO).astype(jnp.int32)
    return dict(coarse_density=coarse_density, fine_density=fine_density, fine_start=fine_start, anchor=anchor)


highest = lax.Precision.HIGHEST

def sine_table(amount):
    indices = jnp.arange(amount, dtype=jnp.int32) + 1
    product = indices[:, None] * indices[None, :] % (2 * (amount + 1))
    angles = product.astype(jnp.float32) * (math.pi / (amount + 1))
    return math.sqrt(2.0 / (amount + 1)) * jnp.sin(angles)

def eigen_values(indices, amount):
    angles = (indices + 1).astype(jnp.float32) * (math.pi / (2 * (amount + 1)))
    return -4.0 * jnp.square(jnp.sin(angles))

def interpolation(fine_index, cell_count):
    scaled = 2 * fine_index + 1 + RATIO
    bottom = scaled // (2 * RATIO)
    weight = (scaled % (2 * RATIO)).astype(jnp.float32) / (2.0 * RATIO)
    column = jnp.arange(cell_count, dtype=jnp.int32)
    first_part = jnp.where(column[None, :] == bottom[:, None], 1.0 - weight[:, None], 0.0)
    second_part = jnp.where(column[None, :] == bottom[:, None] + 1, weight[:, None], 0.0)
    return first_part + second_part

def transform(values, matrix):
    values = jnp.einsum('abc,cd->abd', values, matrix, precision=highest)
    values = jnp.einsum('abc,bd->adc', values, matrix, precision=highest)
    return jnp.einsum('abc,ad->dbc', values, matrix, precision=highest)

def ghost_values(face, left_matrix, right_matrix):
    partial_value = jnp.einsum('fbc,kc->fbk', face, right_matrix, precision=highest)
    return jnp.einsum('fbk,jb->fjk', partial_value, left_matrix, precision=highest)

def reference(coarse_density, fine_density, fine_start, anchor):
    matrix = sine_table(NC)
    eigen_list = eigen_values(jnp.arange(NC, dtype=jnp.int32), NC)
    spectrum = transform(coarse_density, matrix)
    divisor = eigen_list[:, None, None] + eigen_list[None, :, None] + eigen_list[None, None, :]
    potential = transform(spectrum / divisor, matrix)
    coarse_box = lax.dynamic_slice(potential, (anchor[0] - 1, anchor[1] - 1, anchor[2] - 1), (CBX, CBY, CBZ))
    ends_x = interpolation(jnp.array([-1, FX], dtype=jnp.int32), CBX)
    ends_y = interpolation(jnp.array([-1, FY], dtype=jnp.int32), CBY)
    ends_z = interpolation(jnp.array([-1, FZ], dtype=jnp.int32), CBZ)
    inner_x = interpolation(jnp.arange(FX, dtype=jnp.int32), CBX)
    inner_y = interpolation(jnp.arange(FY, dtype=jnp.int32), CBY)
    inner_z = interpolation(jnp.arange(FZ, dtype=jnp.int32), CBZ)
    face_x = jnp.einsum('fa,abc->fbc', ends_x, coarse_box, precision=highest)
    face_y = jnp.einsum('fb,abc->fac', ends_y, coarse_box, precision=highest)
    face_z = jnp.einsum('fc,abc->fab', ends_z, coarse_box, precision=highest)
    ghost_x = ghost_values(face_x, inner_y, inner_z)
    ghost_y = ghost_values(face_y, inner_x, inner_z)
    ghost_z = ghost_values(face_z, inner_x, inner_y)
    padded = jnp.zeros((FX + 2, FY + 2, FZ + 2), jnp.float32)
    padded = padded.at[1:-1, 1:-1, 1:-1].set(fine_start)
    padded = padded.at[0, 1:-1, 1:-1].set(ghost_x[0]).at[-1, 1:-1, 1:-1].set(ghost_x[1])
    padded = padded.at[1:-1, 0, 1:-1].set(ghost_y[0]).at[1:-1, -1, 1:-1].set(ghost_y[1])
    padded = padded.at[1:-1, 1:-1, 0].set(ghost_z[0]).at[1:-1, 1:-1, -1].set(ghost_z[1])
    source = fine_density / (RATIO * RATIO)
    for sweep in range(SWEEPS):
        summed = padded[2:, 1:-1, 1:-1] + padded[:-2, 1:-1, 1:-1]
        summed = summed + padded[1:-1, 2:, 1:-1] + padded[1:-1, :-2, 1:-1]
        summed = summed + padded[1:-1, 1:-1, 2:] + padded[1:-1, 1:-1, :-2]
        padded = padded.at[1:-1, 1:-1, 1:-1].set((summed - source) / 6.0)
    return (potential, padded[1:-1, 1:-1, 1:-1])
```

```python
import functools
import math

import jax
import jax.numpy as jnp
import numpy as np
from jax import lax
from jax.experimental import pallas as pl
from jax.experimental.pallas import tpu as pltpu
from jax.sharding import PartitionSpec as P

RATIO = 4
SWEEPS = 8
EVERY = ("gx", "grp", "gy")
VMEM_LIMIT = 60 * 1024 * 1024

highest = lax.Precision.HIGHEST


def with_halo(block, sides, width):
    for axis, dim in sides:
        count = lax.axis_size(axis)
        forward = [(i, i + 1) for i in range(count - 1)]
        backward = [(target, source) for source, target in forward]
        low = lax.ppermute(
            lax.slice_in_dim(block, block.shape[dim] - width, None, axis=dim), axis, forward
        )
        high_side = lax.ppermute(lax.slice_in_dim(block, 0, width, axis=dim), axis, backward)
        block = jnp.concatenate([low, block, high_side], axis=dim)
    return block


def sine_table(amount):
    indices = np.arange(1, amount + 1, dtype=np.int64)
    product = indices[:, None] * indices[None, :] % (2 * (amount + 1))
    return math.sqrt(2.0 / (amount + 1)) * np.sin(product * (math.pi / (amount + 1)))


def eigen_values(amount):
    return -4.0 * np.square(np.sin(np.arange(1, amount + 1) * (math.pi / (2 * (amount + 1)))))


def parity_order(amount):
    return np.concatenate([np.arange(0, amount, 2), np.arange(1, amount, 2)])


def halves(table):
    top = table.astype(np.float32).astype(jnp.bfloat16)
    rest = (table - top.astype(np.float64)).astype(np.float32).astype(jnp.bfloat16)
    return top, rest


def folded_tables(amount):
    table = sine_table(amount)[: amount // 2]
    even, odd = table[:, 0::2], table[:, 1::2]
    forward, inverse = [], []
    for part in (even, odd):
        top, rest = halves(part)
        forward.append(np.concatenate([top, top, rest], axis=0))
        top, rest = halves(part.T)
        inverse.append(np.concatenate([top, top, rest], axis=0))
    return np.stack(forward), np.stack(inverse)


def decay_table(cols, depth):
    lam_z = eigen_values(depth)[parity_order(depth)]
    size = -(eigen_values(cols)[:, None] + lam_z[None, :])
    return (2.0 / (2.0 + size + np.sqrt(size * (size + 4.0)))).astype(np.float32)


def split(values):
    top = values.astype(jnp.bfloat16)
    return top, (values - top.astype(jnp.float32)).astype(jnp.bfloat16)


def reverse_lanes(values):
    rows, width = values.shape
    tiles = width // 128
    index = 127 - lax.broadcasted_iota(jnp.int32, (rows, 128), 1)
    parts = [
        jnp.take_along_axis(values[:, t * 128 : (t + 1) * 128], index, axis=1)
        for t in reversed(range(tiles))
    ]
    return jnp.concatenate(parts, axis=1)


def dot32(left, right):
    return jnp.dot(left, right, preferred_element_type=jnp.float32)


def triple(values):
    top, rest = split(values)
    return jnp.concatenate([top, rest, top], axis=1)


def cols_transform(sine3, values):
    top, rest = split(values)
    return dot32(sine3, jnp.concatenate([top, rest, top], axis=0))


def forward_kernel(shape, chunk, block, depth_table, sine3, sine, decay, ends, out_w, out_t, w, traces, sems):
    rows, cols, depth = shape
    half = depth // 2
    count = rows // chunk
    step = pl.program_id(0)

    def send(index):
        part = pl.ds(index * chunk, chunk)
        return pltpu.make_async_copy(w.at[part], out_w.at[part], sems.at[index])

    values = block[...].reshape(chunk * cols, depth)
    low = values[:, :half]
    high = reverse_lanes(values[:, half:])
    even = dot32(triple(low + high), depth_table[0])
    odd = dot32(triple(low - high), depth_table[1])
    even = even.reshape(chunk, cols, half)
    odd = odd.reshape(chunk, cols, half)
    rate = decay[...]
    for x in range(chunk):
        here = step * chunk + x
        now = cols_transform(sine3[...], jnp.concatenate([even[x], odd[x]], axis=1))
        if x == 0:
            before = w[jnp.maximum(here - 1, 0)]
            before = jnp.where(step == 0, 0.0, before)
        else:
            before = w[here - 1]
        w[here] = rate * (before - now)

    @pl.when(step > 0)
    def _():
        send(step - 1).start()

    @pl.when(step == count - 1)
    def _():
        send(step).start()
        for tile in range(depth // 128):
            lanes = slice(tile * 128, (tile + 1) * 128)
            rate = decay[:, lanes]
            first = ends[:, 0:1] * jnp.ones((1, 128), jnp.float32)
            second = ends[:, 1:2] * jnp.ones((1, 128), jnp.float32)

            def back(i, value):
                base = pl.multiple_of((rows // 8 - 1 - i) * 8, 8)
                got_first, got_second = [None] * 8, [None] * 8
                for x in reversed(range(8)):
                    value = w[base + x, :, lanes] + rate * value
                    got_first[x] = jnp.sum(value * first, axis=0, keepdims=True)
                    got_second[x] = jnp.sum(value * second, axis=0, keepdims=True)
                traces[pl.ds(3 * cols + base, 8), lanes] = jnp.concatenate(got_first, axis=0)
                traces[pl.ds(3 * cols + rows + base, 8), lanes] = jnp.concatenate(got_second, axis=0)
                return value

            start = lax.fori_loop(0, rows // 8, back, jnp.zeros((cols, 128), jnp.float32))
            for index, plane in enumerate((start, w[rows - 1, :, lanes], rate * start)):
                traces[index * cols : (index + 1) * cols, lanes] = jnp.dot(
                    sine[...], plane, precision=highest, preferred_element_type=jnp.float32
                )
        out_t[...] = traces[...].T
        for index in range(count):
            send(index).wait()


def inverse_kernel(shape, chunk, part, back, depth_table, sine3, sine, decay, ends, out, w, known, carry):
    rows, cols, depth = shape
    half = depth // 2
    count = rows // chunk
    step = pl.program_id(0)

    @pl.when(step == 0)
    def _():
        known[...] = back[...].T
        planes = [
            jnp.dot(
                sine[...],
                known[index * cols : (index + 1) * cols],
                precision=highest,
                preferred_element_type=jnp.float32,
            )
            for index in range(3)
        ]
        carry[0] = planes[0] - decay[...] * planes[2]
        carry[1] = planes[1]

    @pl.when(step < count)
    def _():
        rate = decay[...]
        first = ends[:, 0:1] * jnp.ones((1, depth), jnp.float32)
        second = ends[:, 1:2] * jnp.ones((1, depth), jnp.float32)
        value = carry[0]
        for x in range(chunk):
            here = step * chunk + x
            value = rate * (
                value
                + first * known[pl.ds(3 * cols + here, 1)]
                + second * known[pl.ds(3 * cols + rows + here, 1)]
            )
            w[here] = part[x] + value
        carry[0] = value

    @pl.when(step == count - 1)
    def _():
        w[rows - 1] = w[rows - 1] + decay[...] * carry[1]
        carry[0] = jnp.zeros((cols, depth), jnp.float32)

    @pl.when(step >= count)
    def _():
        base = (2 * count - 1 - step) * chunk
        rate = decay[...]
        value = carry[0]
        planes = [None] * chunk
        for x in reversed(range(chunk)):
            value = w[base + x] + rate * value
            planes[x] = cols_transform(sine3[...], value)
        carry[0] = value
        values = jnp.concatenate(planes, axis=0)
        even = dot32(triple(values[:, :half]), depth_table[0])
        odd = dot32(triple(values[:, half:]), depth_table[1])
        result = jnp.concatenate([even + odd, reverse_lanes(even - odd)], axis=1)
        out[...] = result.reshape(chunk, cols, depth)


def local_tables(shape):
    rows, cols, depth = shape
    forward, inverse = folded_tables(depth)
    sine = sine_table(cols)
    top, rest = halves(sine)
    sine3 = np.concatenate([top, top, rest], axis=1)
    ends = np.stack([sine[:, 0], sine[:, -1]], axis=1).astype(np.float32)
    return forward, inverse, (sine3, sine.astype(np.float32), decay_table(cols, depth), ends)


def full(array):
    return pl.BlockSpec(array.shape, lambda i, rank=array.ndim: (0,) * rank)


def swap_sides(planes):
    inner = planes[1:-1].reshape((-1, 2) + planes.shape[1:])[:, ::-1]
    inner = inner.reshape((-1,) + planes.shape[1:])
    zero = jnp.zeros_like(planes[:1])
    return jnp.concatenate([zero, inner, zero], axis=0)


def coarse_solve(density):
    rows, cols, depth = density.shape
    shape = density.shape
    strips = lax.axis_size("gx")
    bands = lax.axis_size(("grp", "gy"))
    devices = strips * bands
    share = depth // devices
    length_0 = rows * strips
    length_1 = cols * bands
    chunk = 8
    count = rows // chunk
    width = 3 * cols + 2 * rows
    forward, inverse, tables = local_tables(shape)
    params = pltpu.CompilerParams(
        dimension_semantics=("arbitrary",), vmem_limit_bytes=VMEM_LIMIT
    )
    swept, traces = pl.pallas_call(
        functools.partial(forward_kernel, shape, chunk),
        grid=(count,),
        in_specs=[pl.BlockSpec((chunk, cols, depth), lambda i: (i, 0, 0)), full(forward)]
        + [full(table) for table in tables],
        out_specs=[pl.BlockSpec(memory_space=pl.ANY), pl.BlockSpec((depth, width), lambda i: (0, 0))],
        out_shape=[
            jax.ShapeDtypeStruct(shape, jnp.float32),
            jax.ShapeDtypeStruct((depth, width), jnp.float32),
        ],
        scratch_shapes=[
            pltpu.VMEM(shape, jnp.float32),
            pltpu.VMEM((width, depth), jnp.float32),
            pltpu.SemaphoreType.DMA((count,)),
        ],
        compiler_params=params,
        name="local_forward",
    )(density, forward, *tables)

    packed = traces.reshape(devices, share, width)
    packed = lax.all_to_all(packed, EVERY, split_axis=0, concat_axis=0, tiled=True)
    back = middle(packed, rows, cols, strips, bands, depth)
    back = lax.all_to_all(back, EVERY, split_axis=0, concat_axis=0, tiled=True)
    back = back.reshape(depth, width)

    return pl.pallas_call(
        functools.partial(inverse_kernel, shape, chunk),
        grid=(2 * count,),
        in_specs=[
            pl.BlockSpec((chunk, cols, depth), lambda i: (jnp.minimum(i, count - 1), 0, 0)),
            full(back),
            full(inverse),
        ]
        + [full(table) for table in tables],
        out_specs=pl.BlockSpec(
            (chunk, cols, depth), lambda i: (jnp.minimum(2 * count - 1 - i, count - 1), 0, 0)
        ),
        out_shape=jax.ShapeDtypeStruct(shape, jnp.float32),
        scratch_shapes=[
            pltpu.VMEM(shape, jnp.float32),
            pltpu.VMEM((width, depth), jnp.float32),
            pltpu.VMEM((2, cols, depth), jnp.float32),
        ],
        compiler_params=params,
        name="local_inverse",
    )(swept, back, inverse, *tables)


def thirds(values):
    first = values.astype(jnp.bfloat16).astype(jnp.float32)
    rest = values - first
    second = rest.astype(jnp.bfloat16).astype(jnp.float32)
    return first, second, rest - second


def wave_kernel(block, sides_0, sides_1, stack_0, stack_1, source_0, source_1, lam_0, lam_1, lam_z, out_0, out_1):
    length_0 = lam_0.shape[0]
    left = jnp.concatenate([sides_0[...], source_1[0]], axis=0)
    right = jnp.concatenate([source_0[0], sides_1[...]], axis=0)
    a1, a2, a3 = thirds(left)
    b1, b2, b3 = thirds(right)
    left = jnp.concatenate([a1, a1, a2, a1, a2, a3], axis=0)
    right = jnp.concatenate([b1, b2, b1, b3, b2, b1], axis=0).astype(jnp.bfloat16)
    offset = lam_1[...] + lam_z[0]
    count_0, count_1 = sides_0.shape[0], sides_1.shape[0]
    total = jnp.zeros((2 * count_0, lam_1.shape[1]), jnp.float32)
    for start in range(0, length_0, block):
        part = slice(start, start + block)
        wave = dot32(left[:, part].T.astype(jnp.bfloat16), right) / (lam_0[part] + offset)
        top, rest = split(wave)
        total += dot32(stack_0[:, part], top) + dot32(stack_0[:, part], rest)
        dims = (((1,), (1,)), ((), ()))
        other = lax.dot_general(stack_1[...], top, dims, preferred_element_type=jnp.float32)
        other += lax.dot_general(stack_1[...], rest, dims, preferred_element_type=jnp.float32)
        out_1[0, :, part] = other[:count_1] + other[count_1:]
    out_0[0] = total[:count_0] + total[count_0:]


def waves(sides_0, sides_1, source_0, source_1, depth):
    share, count_0, length_1 = source_0.shape
    _, count_1, length_0 = source_1.shape
    lam_z = jnp.asarray(eigen_values(depth)[parity_order(depth)].astype(np.float32))
    lam_z = lax.dynamic_slice(lam_z, (lax.axis_index(EVERY) * share,), (share,))
    lam_z = jnp.broadcast_to(lam_z[:, None, None], (share, 1, 128))[:, :, :1]
    lam_0 = eigen_values(length_0).astype(np.float32)[:, None]
    lam_1 = eigen_values(length_1).astype(np.float32)[None, :]
    stacks = [np.concatenate(halves(table), axis=0) for table in (sides_0, sides_1)]
    sides = [table.astype(np.float32) for table in (sides_0, sides_1)]
    fixed = [*sides, *stacks]
    each = lambda shape: pl.BlockSpec((1,) + shape[1:], lambda i: (i, 0, 0))
    out_shape = [jax.ShapeDtypeStruct(part.shape, jnp.float32) for part in (source_0, source_1)]
    return pl.pallas_call(
        functools.partial(wave_kernel, math.gcd(256, length_0)),
        grid=(share,),
        in_specs=[full(table) for table in fixed]
        + [each(source_0.shape), each(source_1.shape), full(lam_0), full(lam_1), each(lam_z.shape)],
        out_specs=[each(part.shape) for part in out_shape],
        out_shape=out_shape,
        compiler_params=pltpu.CompilerParams(
            dimension_semantics=("arbitrary",), vmem_limit_bytes=VMEM_LIMIT
        ),
        name="waves",
    )(*fixed, source_0, source_1, lam_0, lam_1, lam_z)


def middle(packed, rows, cols, strips, bands, depth):
    devices, share, width = packed.shape
    cut = 2 * cols
    length_0 = rows * strips
    length_1 = cols * bands
    table_0, table_1 = sine_table(length_0), sine_table(length_1)
    full_0 = jnp.asarray(table_0.astype(np.float32))
    full_1 = full_0 if length_1 == length_0 else jnp.asarray(table_1.astype(np.float32))
    planes_0 = packed[:, :, :cut].reshape(strips, bands, share, 2, cols)
    planes_0 = planes_0.transpose(0, 3, 2, 1, 4).reshape(2 * strips, share, length_1)
    scaled = packed[:, :, cut : cut + cols].reshape(strips, bands, share, cols)
    scaled = scaled.transpose(0, 2, 1, 3).reshape(strips, 1, share, length_1)
    scaled = jnp.concatenate([scaled, jnp.zeros_like(scaled)], axis=1).reshape(planes_0.shape)
    planes_1 = packed[:, :, 3 * cols :].reshape(strips, bands, share, 2, rows)
    planes_1 = planes_1.transpose(1, 3, 2, 0, 4).reshape(2 * bands, share, length_0)
    source_0 = jnp.einsum("pkj,jl->kpl", scaled - swap_sides(planes_0), full_1, precision=highest)
    source_1 = jnp.einsum("qkj,jl->kql", -swap_sides(planes_1), full_0, precision=highest)
    sides_0 = table_0.reshape(strips, rows, length_0)[:, [0, rows - 1]].reshape(2 * strips, length_0)
    sides_1 = table_1.reshape(bands, cols, length_1)[:, [0, cols - 1]].reshape(2 * bands, length_1)
    wave_0, wave_1 = waves(sides_0, sides_1, source_0, source_1, depth)
    side_0 = planes_0 + jnp.einsum("kpl,jl->pkj", wave_0, full_1, precision=highest)
    side_1 = planes_1 + jnp.einsum("kql,jl->qkj", wave_1, full_0, precision=highest)
    back_0 = swap_sides(side_0).reshape(strips, 2, share, bands, cols)
    back_0 = back_0.transpose(0, 3, 2, 1, 4).reshape(devices, share, cut)
    own = side_0.reshape(strips, 2, share, bands, cols)[:, 0]
    own = own.transpose(0, 2, 1, 3).reshape(devices, share, cols)
    back_1 = swap_sides(side_1).reshape(bands, 2, share, strips, rows)
    back_1 = back_1.transpose(3, 0, 2, 1, 4).reshape(devices, share, 2 * rows)
    return jnp.concatenate([back_0, own, back_1], axis=2)


def weights(fine_index, cell):
    scaled = 2 * fine_index + 1 + RATIO
    bottom = scaled >> 3
    weight = (scaled & 7).astype(jnp.float32) * 0.125
    return jnp.where(cell == bottom, 1.0 - weight, jnp.where(cell == bottom + 1, weight, 0.0))


def end_weights(total):
    result = []
    for index in (-1, total):
        scaled = 2 * index + 1 + RATIO
        result.append((scaled // (2 * RATIO), (scaled % (2 * RATIO)) / (2.0 * RATIO)))
    return result


class Plan:
    def __init__(self, fine, counts):
        self.fine = fine
        self.counts = counts
        self.totals = tuple(size * count for size, count in zip(fine, counts))
        self.bounds = tuple(total // RATIO + 2 for total in self.totals)
        self.reach = [size // RATIO + 6 for size in fine]
        if counts[2] == 2:
            self.reach[2] -= 2
        self.rows = -(-max(self.reach[1], 2 * self.reach[0]) // 8) * 8
        self.marks = tuple(self.reach[2] * i for i in range(4))

    def start(self, dim, index):
        return index * (self.fine[dim] // RATIO) - 2

    def start_z(self, index):
        first = self.start(2, index)
        last = self.bounds[2] - self.reach[2]
        if isinstance(index, int):
            return min(max(first, 0), last)
        return jnp.clip(first, 0, last)


def iota(shape, dim):
    return lax.broadcasted_iota(jnp.int32, shape, dim)


def exact_dot(left, right):
    return sum(dot32(left, part.astype(jnp.bfloat16)) for part in thirds(right))


def faces_kernel(plan, shape, near, anchor, potential, out, slab, plane, sem):
    rows, cols, depth = shape
    bound_x, bound_y, bound_z = plan.bounds
    reach_x, reach_y, reach_z = plan.reach
    count_x, count_y, count_z = plan.counts
    shift_x = anchor[0] - 1 - lax.axis_index("gx") * rows
    band = lax.axis_index("grp") * count_y + lax.axis_index("gy")
    shift_y = anchor[1] - 1 - band * cols
    base_z = anchor[2] - 1
    from_x = jnp.clip(shift_x, 0, rows - near)
    copy = pltpu.make_async_copy(potential.at[pl.ds(from_x, near)], slab, sem)
    copy.start()

    parts = []
    cell = iota((depth, 128), 0) - base_z
    lane = iota((depth, 128), 1)
    ends_z = end_weights(plan.totals[2])
    edge = jnp.zeros((depth, 128), jnp.float32)
    for e, (bottom, weight) in enumerate(ends_z):
        here = jnp.where(cell == bottom, 1.0 - weight, jnp.where(cell == bottom + 1, weight, 0.0))
        edge = jnp.where((lane - plan.marks[3]) % 2 == e, here, edge)
    edge = jnp.where((lane >= plan.marks[3]) & (lane < plan.marks[3] + 2 * reach_x), edge, 0.0)
    for g in range(count_z):
        want = jnp.full((depth, 128), -1, jnp.int32)
        for i in range(3):
            inside = (lane >= plan.marks[i]) & (lane < plan.marks[i + 1])
            want = jnp.where(inside, lane - plan.marks[i] + plan.start_z(g), want)
        hit = (want >= 0) & (want < bound_z) & (cell == want)
        parts.append(jnp.where(hit, 1.0, edge).astype(jnp.bfloat16))
    select_z = jnp.concatenate(parts, axis=1)

    high = count_y * plan.rows
    cell = iota((high, cols), 1) - shift_y
    row = iota((high, cols), 0)
    want = (row // plan.rows) * (plan.fine[1] // RATIO) - 2 + row % plan.rows
    ok = (want >= 0) & (want < bound_y) & (row % plan.rows < reach_y) & (cell == want)
    select_y = jnp.where(ok, 1.0, 0.0)
    cell = iota((plan.rows, cols), 1) - shift_y
    row = iota((plan.rows, cols), 0)
    edge = jnp.zeros((plan.rows, cols), jnp.float32)
    for e, (bottom, weight) in enumerate(end_weights(plan.totals[1])):
        here = jnp.where(cell == bottom, 1.0 - weight, jnp.where(cell == bottom + 1, weight, 0.0))
        edge = jnp.where((row >= e * reach_x) & (row < (e + 1) * reach_x), here, edge)
    select_y = jnp.concatenate([select_y, edge], axis=0).astype(jnp.bfloat16)

    copy.wait()
    for x in range(near):
        line = sum(dot32(part.astype(jnp.bfloat16), select_z) for part in thirds(slab[x]))
        plane[x] = exact_dot(select_y, line)

    cells = []
    for a in range(bound_x):
        place = shift_x + a - from_x
        ok = (place >= 0) & (place < near)
        got = plane[jnp.clip(place, 0, near - 1)]
        cells.append(jnp.where(ok, got, 0.0))
    ends = []
    for bottom, weight in end_weights(plan.totals[0]):
        ends.append((1.0 - weight) * cells[bottom] + weight * cells[bottom + 1])

    lane = iota((plan.rows, 128), 1)
    row = iota((plan.rows, 128), 0)
    for dx in range(count_x):
        first = plan.start(0, dx)
        for g in range(count_z):
            lanes = slice(g * 128, (g + 1) * 128)
            face_y = jnp.zeros((plan.rows, 128), jnp.float32)
            for t in range(reach_x):
                if 0 <= first + t < bound_x:
                    face_y = jnp.where(row % reach_x == t, cells[first + t][high:, lanes], face_y)
            for dy in range(count_y):
                part = slice(dy * plan.rows, (dy + 1) * plan.rows)
                face_z = jnp.zeros((plan.rows, 128), jnp.float32)
                for t in range(reach_x):
                    if 0 <= first + t < bound_x:
                        face_z = jnp.where(
                            (lane - plan.marks[3]) // 2 == t, cells[first + t][part, lanes], face_z
                        )
                value = jnp.where(
                    lane < plan.marks[1],
                    ends[0][part, lanes],
                    jnp.where(
                        lane < plan.marks[2],
                        ends[1][part, lanes],
                        jnp.where(lane < plan.marks[3], face_y, face_z),
                    ),
                )
                out[(dx * count_z + g) * count_y + dy] = value


def box_faces(plan, potential, anchor):
    shape = potential.shape
    near = min(plan.bounds[0], shape[0])
    devices = math.prod(plan.counts)
    return pl.pallas_call(
        functools.partial(faces_kernel, plan, shape, near),
        in_specs=[pl.BlockSpec(memory_space=pltpu.SMEM), pl.BlockSpec(memory_space=pl.ANY)],
        out_specs=pl.BlockSpec(memory_space=pltpu.VMEM),
        out_shape=jax.ShapeDtypeStruct((devices, plan.rows, 128), jnp.float32),
        scratch_shapes=[
            pltpu.VMEM((near,) + shape[1:], jnp.float32),
            pltpu.VMEM((near, (plan.counts[1] + 1) * plan.rows, plan.counts[2] * 128), jnp.float32),
            pltpu.SemaphoreType.DMA,
        ],
        compiler_params=pltpu.CompilerParams(vmem_limit_bytes=VMEM_LIMIT),
        name="faces",
    )(anchor, potential)


def sweep_kernel(plan, width, faces, own, other, out, source, values):
    rows, cols, depth = (size + 2 * width for size in plan.fine)
    depth = 2 * plan.fine[2]
    reach_x, reach_y, reach_z = plan.reach
    total_x, total_y, total_z = plan.totals
    me_x, me_y, me_z = (lax.axis_index(axis) for axis in ("gx", "gy", "grp"))
    at_x = me_x * plan.fine[0] - width
    at_y = me_y * plan.fine[1] - width
    face = jnp.sum(faces[...], axis=0)

    def dot(left, right):
        return jnp.dot(left, right, precision=highest, preferred_element_type=jnp.float32)

    cell = iota((128, depth), 0)
    fine = iota((128, depth), 1)
    expand = []
    for i in range(3):
        place = cell - plan.marks[i]
        table = weights(fine, place + plan.start_z(me_z))
        expand.append(jnp.where((place >= 0) & (place < reach_z), table, 0.0))
    shape = (cols, plan.rows)
    cell = iota(shape, 1)
    table = weights(iota(shape, 0) + at_y, cell + plan.start(1, me_y))
    inner_y = jnp.where(cell < reach_y, table, 0.0)
    shape = (rows, plan.rows)
    cell = iota(shape, 1)
    inner_x = []
    for e in range(2):
        place = cell - e * reach_x
        table = weights(iota(shape, 0) + at_x, place + plan.start(0, me_x))
        inner_x.append(jnp.where((place >= 0) & (place < reach_x), table, 0.0))
    cell = iota((128, 128), 0) - plan.marks[3]
    fine = iota((128, 128), 1)
    edge_x = []
    for e in range(2):
        table = weights(fine + at_x, (cell >> 1) + plan.start(0, me_x))
        edge_x.append(jnp.where((cell >= 0) & (cell < 2 * reach_x) & ((cell & 1) == e), table, 0.0))

    ghost_x = [dot(inner_y, dot(face, expand[e])) for e in range(2)]
    lines = dot(face, expand[2])
    ghost_y = [dot(inner_x[e], lines) for e in range(2)]
    column = dot(inner_y, face)
    ghost_z = [dot(column, edge_x[e]) for e in range(2)]

    y = iota((cols, depth), 0) + at_y
    z = iota((cols, depth), 1)
    scale = jnp.where((y >= 0) & (y < total_y), 1.0 / 6.0, 0.0)

    def whole(index, x):
        mine, theirs = own[index, x], other[index, x]
        left = jnp.where(me_z == 0, mine, theirs)
        right = jnp.where(me_z == 0, theirs, mine)
        return jnp.concatenate([left, right], axis=1)

    for x in range(rows):
        here = at_x + x
        value = whole(0, x) * (-1.0 / (RATIO * RATIO))
        value += jnp.where(here == 0, ghost_x[0], 0.0) + jnp.where(here == total_x - 1, ghost_x[1], 0.0)
        value += jnp.where(y == 0, ghost_y[0][x : x + 1], 0.0)
        value += jnp.where(y == total_y - 1, ghost_y[1][x : x + 1], 0.0)
        value += jnp.where(z == 0, ghost_z[0][:, x : x + 1], 0.0)
        value += jnp.where(z == total_z - 1, ghost_z[1][:, x : x + 1], 0.0)
        source[x] = value
        values[0, x] = whole(1, x)

    for sweep in range(width):
        now, later = sweep % 2, (sweep + 1) % 2
        margin = sweep + 1

        def step(x, carry):
            here = at_x + x
            value = values[now, x]
            total = values[now, x - 1] + values[now, x + 1]
            total += pltpu.roll(value, 1, 0) + pltpu.roll(value, cols - 1, 0)
            total += jnp.where(z == 0, 0.0, pltpu.roll(value, 1, 1))
            total += jnp.where(z == depth - 1, 0.0, pltpu.roll(value, depth - 1, 1))
            keep = jnp.where((here >= 0) & (here < total_x), 1.0, 0.0)
            values[later, x] = (total + source[x]) * (scale * keep)
            return carry

        lax.fori_loop(margin, rows - margin, step, 0)

    for x in range(plan.fine[0]):
        value = values[width % 2, width + x, width : cols - width]
        half = plan.fine[2]
        out[x] = jnp.where(me_z == 0, value[:, :half], value[:, half:])


def body(coarse_density, fine_density, fine_start, anchor):
    fine = fine_start.shape
    counts = tuple(lax.axis_size(axis) for axis in ("gx", "gy", "grp"))
    plan = Plan(fine, counts)
    width = SWEEPS
    both = jnp.stack([fine_density, fine_start])
    both = with_halo(both, (("gx", 1), ("gy", 2)), width)
    other = lax.ppermute(both, "grp", [(0, 1), (1, 0)])

    potential = coarse_solve(coarse_density)
    faces = box_faces(plan, potential, anchor)
    faces = lax.all_to_all(faces, EVERY, split_axis=0, concat_axis=0, tiled=True)
    padded = (fine[0] + 2 * width, fine[1] + 2 * width, 2 * fine[2])
    values = pl.pallas_call(
        functools.partial(sweep_kernel, plan, width),
        out_shape=jax.ShapeDtypeStruct(fine, jnp.float32),
        in_specs=[pl.BlockSpec(memory_space=pltpu.VMEM)] * 3,
        out_specs=pl.BlockSpec(memory_space=pltpu.VMEM),
        scratch_shapes=[pltpu.VMEM(padded, jnp.float32), pltpu.VMEM((2,) + padded, jnp.float32)],
        compiler_params=pltpu.CompilerParams(vmem_limit_bytes=VMEM_LIMIT),
        name="sweeps",
    )(faces, both, other)
    return (potential, values)


def solution(mesh):
    return jax.shard_map(
        body,
        mesh=mesh,
        in_specs=(P("gx", ("grp", "gy"), None), P("gx", "gy", "grp"), P("gx", "gy", "grp"), P()),
        out_specs=(P("gx", ("grp", "gy"), None), P("gx", "gy", "grp")),
        check_vma=False,
    )
```

```python
import functools
import math

import jax
import jax.numpy as jnp
import numpy as np
from jax import lax
from jax.experimental import pallas as pl
from jax.experimental.pallas import tpu as pltpu
from jax.sharding import PartitionSpec as P


RATIO = 4
SWEEPS = 8
EVERY = ("gx", "grp", "gy")
VMEM_LIMIT = 60 * 1024 * 1024

highest = lax.Precision.HIGHEST


def with_halo(block, axis, dim, width):
    count = lax.axis_size(axis)
    forward = [(i, i + 1) for i in range(count - 1)]
    backward = [(target, source) for source, target in forward]
    low = lax.ppermute(
        lax.slice_in_dim(block, block.shape[dim] - width, None, axis=dim), axis, forward
    )
    high = lax.ppermute(lax.slice_in_dim(block, 0, width, axis=dim), axis, backward)
    return jnp.concatenate([low, block, high], axis=dim)


def sine_table(amount):
    indices = np.arange(1, amount + 1, dtype=np.int64)
    product = indices[:, None] * indices[None, :] % (2 * (amount + 1))
    return math.sqrt(2.0 / (amount + 1)) * np.sin(product * (math.pi / (amount + 1)))


def eigen_values(amount):
    return -4.0 * np.square(np.sin(np.arange(1, amount + 1) * (math.pi / (2 * (amount + 1)))))


def parity_order(amount):
    return np.concatenate([np.arange(0, amount, 2), np.arange(1, amount, 2)])


def halves(table):
    top = table.astype(np.float32).astype(jnp.bfloat16)
    rest = (table - top.astype(np.float64)).astype(np.float32).astype(jnp.bfloat16)
    return top, rest


def folded_tables(amount):
    table = sine_table(amount)[: amount // 2]
    even, odd = table[:, 0::2], table[:, 1::2]
    forward, inverse = [], []
    for part in (even, odd):
        top, rest = halves(part)
        forward.append(np.concatenate([top, top, rest], axis=0))
        top, rest = halves(part.T)
        inverse.append(np.concatenate([top, top, rest], axis=0))
    return np.stack(forward), np.stack(inverse)


def decay_table(cols, depth):
    lam_z = eigen_values(depth)[parity_order(depth)]
    size = -(eigen_values(cols)[:, None] + lam_z[None, :])
    return (2.0 / (2.0 + size + np.sqrt(size * (size + 4.0)))).astype(np.float32)


def split(values):
    top = values.astype(jnp.bfloat16)
    return top, (values - top.astype(jnp.float32)).astype(jnp.bfloat16)


def reverse_lanes(values):
    rows, width = values.shape
    tiles = width // 128
    index = 127 - lax.broadcasted_iota(jnp.int32, (rows, 128), 1)
    parts = [
        jnp.take_along_axis(values[:, t * 128 : (t + 1) * 128], index, axis=1)
        for t in reversed(range(tiles))
    ]
    return jnp.concatenate(parts, axis=1)


def dot32(left, right):
    return jnp.dot(left, right, preferred_element_type=jnp.float32)


def triple(values):
    top, rest = split(values)
    return jnp.concatenate([top, rest, top], axis=1)


def cols_transform(sine3, values):
    top, rest = split(values)
    return dot32(sine3, jnp.concatenate([top, rest, top], axis=0))


def forward_kernel(shape, chunk, block, depth_table, sine3, sine, decay, ends, out_w, *rest):
    rows, cols, depth = shape
    half = depth // 2
    count = rows // chunk
    step = pl.program_id(0)
    *out_t, w, traces, sems, loads = rest

    def send(index):
        part = pl.ds(index * chunk, chunk)
        return pltpu.make_async_copy(w.at[part], out_w.at[part], sems.at[index])

    def load(index):
        part = pl.ds(index * chunk, chunk)
        return pltpu.make_async_copy(block.at[part], w.at[part], loads.at[index])

    @pl.when(step == 0)
    def _():
        for index in range(count):
            load(index).start()

    load(step).wait()
    values = w[pl.ds(step * chunk, chunk)].reshape(chunk * cols, depth)
    low = values[:, :half]
    high = reverse_lanes(values[:, half:])
    even = dot32(triple(low + high), depth_table[0])
    odd = dot32(triple(low - high), depth_table[1])
    even = even.reshape(chunk, cols, half)
    odd = odd.reshape(chunk, cols, half)
    rate = decay[...]
    for x in range(chunk):
        here = step * chunk + x
        now = cols_transform(sine3[...], jnp.concatenate([even[x], odd[x]], axis=1))
        if x == 0:
            before = w[jnp.maximum(here - 1, 0)]
            before = jnp.where(step == 0, 0.0, before)
        else:
            before = w[here - 1]
        w[here] = rate * (before - now)

    @pl.when(step > 0)
    def _():
        send(step - 1).start()

    @pl.when(step == count - 1)
    def _():
        send(step).start()
        for tile in range(depth // 128):
            lanes = slice(tile * 128, (tile + 1) * 128)
            rate = decay[:, lanes]
            first = ends[:, 0:1] * jnp.ones((1, 128), jnp.float32)
            second = ends[:, 1:2] * jnp.ones((1, 128), jnp.float32)

            def back(i, value):
                base = pl.multiple_of((rows // 8 - 1 - i) * 8, 8)
                got_first, got_second = [None] * 8, [None] * 8
                for x in reversed(range(8)):
                    value = w[base + x, :, lanes] + rate * value
                    got_first[x] = jnp.sum(value * first, axis=0, keepdims=True)
                    got_second[x] = jnp.sum(value * second, axis=0, keepdims=True)
                traces[pl.ds(base, 8), lanes] = jnp.concatenate(got_first, axis=0)
                traces[pl.ds(rows + base, 8), lanes] = jnp.concatenate(got_second, axis=0)
                return value

            start = lax.fori_loop(0, rows // 8, back, jnp.zeros((cols, 128), jnp.float32))
            for index, plane in enumerate((start, w[rows - 1, :, lanes])):
                top = 2 * rows + index * cols
                traces[top : top + cols, lanes] = jnp.dot(
                    sine[...], plane, precision=highest, preferred_element_type=jnp.float32
                )
        size = depth // len(out_t)
        for index, target in enumerate(out_t):
            target[...] = traces[:, index * size : (index + 1) * size].T
        for index in range(count):
            send(index).wait()


def inverse_kernel(shape, chunk, parts, swept, *rest):
    rows, cols, depth = shape
    half = depth // 2
    count = rows // chunk
    step = pl.program_id(0)
    back, rest = rest[:parts], rest[parts:]
    depth_table, sine3, sine, decay, ends, out, w, known, carry, sems, loads = rest

    def load(index):
        part = pl.ds(index * chunk, chunk)
        return pltpu.make_async_copy(swept.at[part], w.at[part], loads.at[index])

    def send(index):
        part = pl.ds(index * chunk, chunk)
        return pltpu.make_async_copy(w.at[part], out.at[part], sems.at[index])

    @pl.when(step == 0)
    def _():
        for index in range(count):
            load(index).start()
        size = depth // parts
        for index in range(parts):
            known[:, index * size : (index + 1) * size] = back[index][...].T
        planes = [
            jnp.dot(
                sine[...],
                known[2 * rows + index * cols : 2 * rows + (index + 1) * cols],
                precision=highest,
                preferred_element_type=jnp.float32,
            )
            for index in range(2)
        ]
        carry[0] = planes[0]
        carry[1] = planes[1]

    @pl.when(step < count)
    def _():
        rate = decay[...]
        first = ends[:, 0:1] * jnp.ones((1, depth), jnp.float32)
        second = ends[:, 1:2] * jnp.ones((1, depth), jnp.float32)
        value = carry[0]
        load(step).wait()
        for x in range(chunk):
            here = step * chunk + x
            value = rate * (
                value
                + first * known[pl.ds(here, 1)]
                + second * known[pl.ds(rows + here, 1)]
            )
            w[here] = w[here] + value
        carry[0] = value

    @pl.when(step == count - 1)
    def _():
        w[rows - 1] = w[rows - 1] + decay[...] * carry[1]
        carry[0] = jnp.zeros((cols, depth), jnp.float32)

    @pl.when(step >= count)
    def _():
        place = 2 * count - 1 - step
        base = place * chunk
        rate = decay[...]
        value = carry[0]
        planes = [None] * chunk
        for x in reversed(range(chunk)):
            value = w[base + x] + rate * value
            planes[x] = cols_transform(sine3[...], value)
        carry[0] = value
        values = jnp.concatenate(planes, axis=0)
        even = dot32(triple(values[:, :half]), depth_table[0])
        odd = dot32(triple(values[:, half:]), depth_table[1])
        result = jnp.concatenate([even + odd, reverse_lanes(even - odd)], axis=1)
        w[pl.ds(base, chunk)] = result.reshape(chunk, cols, depth)

        @pl.when(step > count)
        def _():
            send(place + 1).start()

        @pl.when(step == 2 * count - 1)
        def _():
            send(place).start()
            for index in range(count):
                send(index).wait()


def local_tables(shape):
    _, cols, depth = shape
    forward, inverse = folded_tables(depth)
    sine = sine_table(cols)
    top, rest = halves(sine)
    sine3 = np.concatenate([top, top, rest], axis=1)
    ends = np.stack([sine[:, 0], sine[:, -1]], axis=1).astype(np.float32)
    return forward, inverse, (sine3, sine.astype(np.float32), decay_table(cols, depth), ends)


def full(array):
    return pl.BlockSpec(array.shape, lambda i, rank=array.ndim: (0,) * rank)


def coarse_solve(density):
    rows, cols, depth = density.shape
    shape = density.shape
    strips = lax.axis_size("gx")
    bands = lax.axis_size(("grp", "gy"))
    devices = strips * bands
    parts = 2 if depth % (16 * devices) == 0 else 1
    share = depth // (devices * parts)
    chunk = 16
    count = rows // chunk
    width = 2 * cols + 2 * rows
    forward, inverse, tables = local_tables(shape)
    params = pltpu.CompilerParams(
        dimension_semantics=("arbitrary",), vmem_limit_bytes=VMEM_LIMIT
    )
    swept, *traces = pl.pallas_call(
        functools.partial(forward_kernel, shape, chunk),
        grid=(count,),
        in_specs=[pl.BlockSpec(memory_space=pl.ANY), full(forward)]
        + [full(table) for table in tables],
        out_specs=[pl.BlockSpec(memory_space=pl.ANY)]
        + [pl.BlockSpec((depth // parts, width), lambda i: (0, 0))] * parts,
        out_shape=[jax.ShapeDtypeStruct(shape, jnp.float32)]
        + [jax.ShapeDtypeStruct((depth // parts, width), jnp.float32)] * parts,
        scratch_shapes=[
            pltpu.VMEM(shape, jnp.float32),
            pltpu.VMEM((width, depth), jnp.float32),
            pltpu.SemaphoreType.DMA((count,)),
            pltpu.SemaphoreType.DMA((count,)),
        ],
        compiler_params=params,
        cost_estimate=cost(30e9),
        name="local_forward",
    )(density, forward, *tables)

    back = []
    for index in range(parts):
        packed = lax.all_to_all(
            traces[index].reshape(devices, share, width), EVERY, split_axis=0, concat_axis=0, tiled=True
        )
        sides = middle(packed, rows, cols, strips, bands, depth, index * devices * share)
        sides = lax.all_to_all(sides, EVERY, split_axis=0, concat_axis=0, tiled=True)
        back.append(sides.reshape(depth // parts, width))

    return pl.pallas_call(
        functools.partial(inverse_kernel, shape, chunk, parts),
        grid=(2 * count,),
        in_specs=[
            pl.BlockSpec(memory_space=pl.ANY),
            *[full(part) for part in back],
            full(inverse),
        ]
        + [full(table) for table in tables],
        out_specs=pl.BlockSpec(memory_space=pl.ANY),
        out_shape=jax.ShapeDtypeStruct(shape, jnp.float32),
        scratch_shapes=[
            pltpu.VMEM(shape, jnp.float32),
            pltpu.VMEM((width, depth), jnp.float32),
            pltpu.VMEM((2, cols, depth), jnp.float32),
            pltpu.SemaphoreType.DMA((count,)),
            pltpu.SemaphoreType.DMA((count,)),
        ],
        compiler_params=params,
        cost_estimate=cost(30e9),
        name="local_inverse",
    )(swept, *back, inverse, *tables)


def thirds(values):
    first = values.astype(jnp.bfloat16).astype(jnp.float32)
    rest = values - first
    second = rest.astype(jnp.bfloat16).astype(jnp.float32)
    return first, second, rest - second


def middle_tables(rows, cols, strips, bands, share):
    count_0, count_1 = 2 * strips, 2 * bands
    table_0, table_1 = sine_table(rows * strips), sine_table(cols * bands)

    def stacked(table):
        top, rest = halves(table)
        return np.concatenate([top, top, rest], axis=0)

    def ends(table, count, size):
        picked = table.reshape(count, size, -1)[:, [0, size - 1]].reshape(2 * count, -1)
        return picked.astype(np.float32), np.concatenate(halves(picked), axis=0)

    def shuffle(count, swap):
        matrix = np.zeros((count * share, count * share), np.float32)
        for plane in range(count):
            other = plane if not swap else ((plane - 1) ^ 1) + 1
            if 0 <= other < count:
                for k in range(share):
                    matrix[k * count + plane, other * share + k] = 1.0
        return matrix

    blocks = np.kron(np.eye(128 // cols), sine_table(cols))
    gather_0 = shuffle(count_0, False).astype(jnp.bfloat16)
    gather_1 = -shuffle(count_1, True)
    scatter_1 = -gather_1.T
    tables = [stacked(table_0)]
    if rows * strips != cols * bands:
        tables.append(stacked(table_1))
    return (
        *tables,
        stacked(blocks),
        *ends(table_0, strips, rows),
        *ends(table_1, bands, cols),
        gather_0,
        np.ascontiguousarray(gather_0.T),
        gather_1.astype(jnp.bfloat16),
        np.ascontiguousarray(scatter_1).astype(jnp.bfloat16),
        eigen_values(rows * strips).astype(np.float32)[:, None],
        eigen_values(cols * bands).astype(np.float32)[None, :],
        np.tile(eigen_values(cols), bands).astype(np.float32)[None, :],
    )


def middle_kernel(
    sizes, block, packed, lam_own, full_0, *more,
):
    full_1, more = (full_0, more) if sizes[0] * sizes[2] == sizes[1] * sizes[3] else (more[0], more[1:])
    interfaces(sizes, block, packed, lam_own, full_0, full_1, *more)


def interfaces(
    sizes, block, packed, lam_own, full_0, full_1, blocks, sides_0, stack_0, sides_1, stack_1,
    gather_0, scatter_0, gather_1, scatter_1, lam_0, lam_1, lam_y, out, source_0, source_1, wave_0, wave_1, planes_0, planes_1,
):
    rows, cols, strips, bands, share = sizes
    count_0, count_1 = 2 * strips, 2 * bands
    step = pl.program_id(0)

    def swapped(plane, count):
        other = ((plane - 1) ^ 1) + 1
        return other if 0 <= other < count else None

    def scaled(values):
        size = -(lam_y[...] + lam_own[...])
        rate = 2.0 / (2.0 + size + jnp.sqrt(size * (size + 4.0)))
        rate = jnp.concatenate([rate] * strips, axis=0)
        result = []
        for start in range(0, lam_y.shape[1], 128):
            part = slice(start, start + 128)
            value = dot32(triple(values[:, part]), blocks[...]) * rate[:, part]
            result.append(dot32(triple(value), blocks[...]))
        return jnp.concatenate(result, axis=1)

    def line(values, plane):
        return values[plane * share : (plane + 1) * share]

    @pl.when(step == 0)
    def _():
        for b in range(bands):
            for e in range(2):
                lanes = slice(e * rows, (e + 1) * rows)
                parts = [packed[s * bands + b, :, lanes] for s in range(strips)]
                plane = 2 * b + e
                planes_1[plane * share : (plane + 1) * share] = jnp.concatenate(parts, axis=1)
        for s in range(strips):
            for e in range(2):
                lanes = slice(2 * rows + e * cols, 2 * rows + (e + 1) * cols)
                parts = [packed[s * bands + b, :, lanes] for b in range(bands)]
                plane = 2 * s + e
                planes_0[plane * share : (plane + 1) * share] = jnp.concatenate(parts, axis=1)
        value = planes_0[...]
        own = scaled(jnp.concatenate([line(value, 2 * s) for s in range(strips)], axis=0))
        parts = []
        for plane in range(count_0):
            part = jnp.zeros_like(line(value, 0))
            other = swapped(plane, count_0)
            if other is not None:
                part = part - line(value, other)
            if plane % 2 == 0:
                part = part + line(own, plane // 2)
            parts.append(part)
        value = exact_dot(gather_0[...], jnp.concatenate(parts, axis=0))
        source_0[...] = dot32(triple(value), full_1[...]).reshape(source_0.shape)
        value = exact_dot(gather_1[...], planes_1[...])
        source_1[...] = dot32(triple(value), full_0[...]).reshape(source_1.shape)

    left = jnp.concatenate([sides_0[...], source_1[step]], axis=0)
    right = jnp.concatenate([source_0[step], sides_1[...]], axis=0)
    a1, a2 = split(left)
    b1, b2 = split(right)
    a1, a2 = a1.astype(jnp.float32), a2.astype(jnp.float32)
    left = jnp.concatenate([a1, a1, a2], axis=0)
    right = jnp.concatenate([b1.astype(jnp.float32), b2.astype(jnp.float32), b1.astype(jnp.float32)], axis=0)
    right = right.astype(jnp.bfloat16)
    offset = lam_1[...] + lam_own[pl.ds(step, 1)]
    total = jnp.zeros((2 * count_0, lam_1.shape[1]), jnp.float32)
    dims = (((1,), (1,)), ((), ()))
    for start in range(0, lam_0.shape[0], block):
        part = slice(start, start + block)
        wave = dot32(left[:, part].T.astype(jnp.bfloat16), right) / (lam_0[part] + offset)
        top, rest = split(wave)
        total += dot32(stack_0[:, part], top) + dot32(stack_0[:, part], rest)
        other = lax.dot_general(stack_1[...], top, dims, preferred_element_type=jnp.float32)
        other += lax.dot_general(stack_1[...], rest, dims, preferred_element_type=jnp.float32)
        wave_1[step, :, part] = other[:count_1] + other[count_1:]
    wave_0[step] = total[:count_0] + total[count_0:]

    @pl.when(step == share - 1)
    def _():
        value = dot32(triple(wave_0[...].reshape(share * count_0, -1)), full_1[...])
        value = planes_0[...] + exact_dot(scatter_0[...], value)
        own = scaled(jnp.concatenate([line(value, 2 * s) for s in range(strips)], axis=0))
        edge_0 = []
        for plane in range(count_0):
            part = jnp.zeros_like(line(value, 0))
            other = swapped(plane, count_0)
            if other is not None:
                part = part + line(value, other)
            if plane % 2 == 0:
                part = part - line(own, plane // 2)
            edge_0.append(part)
        value = dot32(triple(wave_1[...].reshape(share * count_1, -1)), full_0[...])
        value = exact_dot(scatter_1[...], value)
        edge_1 = []
        for plane in range(count_1):
            part = line(value, plane)
            other = swapped(plane, count_1)
            if other is not None:
                part = part + planes_1[other * share : (other + 1) * share]
            edge_1.append(part)
        for s in range(strips):
            for b in range(bands):
                parts = [edge_1[2 * b + e][:, s * rows : (s + 1) * rows] for e in range(2)]
                parts += [edge_0[2 * s + e][:, b * cols : (b + 1) * cols] for e in range(2)]
                out[s * bands + b] = jnp.concatenate(parts, axis=1)


def middle(packed, rows, cols, strips, bands, depth, offset):
    _, share, _ = packed.shape
    sizes = (rows, cols, strips, bands, share)
    lam = jnp.asarray(eigen_values(depth)[parity_order(depth)].astype(np.float32))
    lam = lax.dynamic_slice(lam, (offset + lax.axis_index(EVERY) * share,), (share,))
    tables = middle_tables(*sizes)
    length_0, length_1 = rows * strips, cols * bands
    return pl.pallas_call(
        functools.partial(middle_kernel, sizes, math.gcd(512, length_0)),
        grid=(share,),
        in_specs=[
            full(packed),
            pl.BlockSpec((share, 1), lambda i: (0, 0)),
        ]
        + [full(table) for table in tables],
        out_specs=pl.BlockSpec(packed.shape, lambda i: (0, 0, 0)),
        out_shape=jax.ShapeDtypeStruct(packed.shape, jnp.float32),
        scratch_shapes=[
            pltpu.VMEM((share, 2 * strips, length_1), jnp.float32),
            pltpu.VMEM((share, 2 * bands, length_0), jnp.float32),
            pltpu.VMEM((share, 2 * strips, length_1), jnp.float32),
            pltpu.VMEM((share, 2 * bands, length_0), jnp.float32),
            pltpu.VMEM((2 * strips * share, length_1), jnp.float32),
            pltpu.VMEM((2 * bands * share, length_0), jnp.float32),
        ],
        compiler_params=pltpu.CompilerParams(
            dimension_semantics=("arbitrary",), vmem_limit_bytes=VMEM_LIMIT
        ),
        cost_estimate=cost(20e9),
        name="interfaces",
    )(packed, lam.reshape(share, 1), *tables)


def cost(flops):
    return pl.CostEstimate(flops=int(flops), bytes_accessed=1 << 24, transcendentals=0)


def weights(fine_index, cell):
    scaled = 2 * fine_index + 1 + RATIO
    bottom = scaled >> 3
    weight = (scaled & 7).astype(jnp.float32) * 0.125
    return jnp.where(cell == bottom, 1.0 - weight, jnp.where(cell == bottom + 1, weight, 0.0))


def end_weights(total):
    result = []
    for index in (-1, total):
        scaled = 2 * index + 1 + RATIO
        result.append((scaled // (2 * RATIO), (scaled % (2 * RATIO)) / (2.0 * RATIO)))
    return result


class Plan:
    def __init__(self, fine, counts):
        self.fine = fine
        self.counts = counts
        self.totals = tuple(size * count for size, count in zip(fine, counts))
        self.bounds = tuple(total // RATIO + 2 for total in self.totals)
        self.reach = [size // RATIO + 6 for size in fine]
        if counts[2] == 2:
            self.reach[2] -= 2
        self.rows = -(-max(self.reach[1], 2 * self.reach[0]) // 8) * 8
        self.marks = tuple(self.reach[2] * i for i in range(4))

    def start(self, dim, index):
        return index * (self.fine[dim] // RATIO) - 2

    def start_z(self, index):
        first = self.start(2, index)
        last = self.bounds[2] - self.reach[2]
        if isinstance(index, int):
            return min(max(first, 0), last)
        return jnp.clip(first, 0, last)


def iota(shape, dim):
    return lax.broadcasted_iota(jnp.int32, shape, dim)


def exact_dot(left, right):
    return sum(dot32(left, part.astype(jnp.bfloat16)) for part in thirds(right))


def faces_kernel(plan, shape, near, anchor, potential, out, slab, plane, sem):
    rows, cols, depth = shape
    bound_x, bound_y, bound_z = plan.bounds
    reach_x, reach_y, _ = plan.reach
    count_x, count_y, count_z = plan.counts
    shift_x = anchor[0] - 1 - lax.axis_index("gx") * rows
    band = lax.axis_index("grp") * count_y + lax.axis_index("gy")
    shift_y = anchor[1] - 1 - band * cols
    base_z = anchor[2] - 1
    from_x = jnp.clip(shift_x, 0, rows - near)
    copy = pltpu.make_async_copy(potential.at[pl.ds(from_x, near)], slab, sem)
    copy.start()

    parts = []
    cell = iota((depth, 128), 0) - base_z
    lane = iota((depth, 128), 1)
    ends_z = end_weights(plan.totals[2])
    edge = jnp.zeros((depth, 128), jnp.float32)
    for e, (bottom, weight) in enumerate(ends_z):
        here = jnp.where(cell == bottom, 1.0 - weight, jnp.where(cell == bottom + 1, weight, 0.0))
        edge = jnp.where((lane - plan.marks[3]) % 2 == e, here, edge)
    edge = jnp.where((lane >= plan.marks[3]) & (lane < plan.marks[3] + 2 * reach_x), edge, 0.0)
    for g in range(count_z):
        want = jnp.full((depth, 128), -1, jnp.int32)
        for i in range(3):
            inside = (lane >= plan.marks[i]) & (lane < plan.marks[i + 1])
            want = jnp.where(inside, lane - plan.marks[i] + plan.start_z(g), want)
        hit = (want >= 0) & (want < bound_z) & (cell == want)
        parts.append(jnp.where(hit, 1.0, edge).astype(jnp.bfloat16))
    select_z = jnp.concatenate(parts, axis=1)

    high = count_y * plan.rows
    cell = iota((high, cols), 1) - shift_y
    row = iota((high, cols), 0)
    want = (row // plan.rows) * (plan.fine[1] // RATIO) - 2 + row % plan.rows
    ok = (want >= 0) & (want < bound_y) & (row % plan.rows < reach_y) & (cell == want)
    select_y = jnp.where(ok, 1.0, 0.0)
    cell = iota((plan.rows, cols), 1) - shift_y
    row = iota((plan.rows, cols), 0)
    edge = jnp.zeros((plan.rows, cols), jnp.float32)
    for e, (bottom, weight) in enumerate(end_weights(plan.totals[1])):
        here = jnp.where(cell == bottom, 1.0 - weight, jnp.where(cell == bottom + 1, weight, 0.0))
        edge = jnp.where((row >= e * reach_x) & (row < (e + 1) * reach_x), here, edge)
    select_y = jnp.concatenate([select_y, edge], axis=0).astype(jnp.bfloat16)

    copy.wait()
    for x in range(near):
        line = sum(dot32(part.astype(jnp.bfloat16), select_z) for part in thirds(slab[x]))
        plane[x] = exact_dot(select_y, line)

    cells = []
    for a in range(bound_x):
        place = shift_x + a - from_x
        ok = (place >= 0) & (place < near)
        got = plane[jnp.clip(place, 0, near - 1)]
        cells.append(jnp.where(ok, got, 0.0))
    ends = []
    for bottom, weight in end_weights(plan.totals[0]):
        ends.append((1.0 - weight) * cells[bottom] + weight * cells[bottom + 1])

    lane = iota((plan.rows, 128), 1)
    row = iota((plan.rows, 128), 0)
    for dx in range(count_x):
        first = plan.start(0, dx)
        for g in range(count_z):
            lanes = slice(g * 128, (g + 1) * 128)
            face_y = jnp.zeros((plan.rows, 128), jnp.float32)
            for t in range(reach_x):
                if 0 <= first + t < bound_x:
                    face_y = jnp.where(row % reach_x == t, cells[first + t][high:, lanes], face_y)
            for dy in range(count_y):
                part = slice(dy * plan.rows, (dy + 1) * plan.rows)
                face_z = jnp.zeros((plan.rows, 128), jnp.float32)
                for t in range(reach_x):
                    if 0 <= first + t < bound_x:
                        face_z = jnp.where(
                            (lane - plan.marks[3]) // 2 == t, cells[first + t][part, lanes], face_z
                        )
                value = jnp.where(
                    lane < plan.marks[1],
                    ends[0][part, lanes],
                    jnp.where(
                        lane < plan.marks[2],
                        ends[1][part, lanes],
                        jnp.where(lane < plan.marks[3], face_y, face_z),
                    ),
                )
                out[(dx * count_z + g) * count_y + dy] = value


def box_faces(plan, potential, anchor):
    shape = potential.shape
    near = min(plan.bounds[0], shape[0])
    devices = math.prod(plan.counts)
    return pl.pallas_call(
        functools.partial(faces_kernel, plan, shape, near),
        in_specs=[pl.BlockSpec(memory_space=pltpu.SMEM), pl.BlockSpec(memory_space=pl.ANY)],
        out_specs=pl.BlockSpec(memory_space=pltpu.VMEM),
        out_shape=jax.ShapeDtypeStruct((devices, plan.rows, 128), jnp.float32),
        scratch_shapes=[
            pltpu.VMEM((near,) + shape[1:], jnp.float32),
            pltpu.VMEM((near, (plan.counts[1] + 1) * plan.rows, plan.counts[2] * 128), jnp.float32),
            pltpu.SemaphoreType.DMA,
        ],
        compiler_params=pltpu.CompilerParams(vmem_limit_bytes=VMEM_LIMIT),
        name="faces",
    )(anchor, potential)


def sweep_kernel(plan, width, faces, own, other, out, source, values):
    rows, cols, depth = (size + 2 * width for size in plan.fine)
    depth = 2 * plan.fine[2]
    reach_x, reach_y, reach_z = plan.reach
    total_x, total_y, total_z = plan.totals
    me_x, me_y, me_z = (lax.axis_index(axis) for axis in ("gx", "gy", "grp"))
    at_x = me_x * plan.fine[0] - width
    at_y = me_y * plan.fine[1] - width
    face = jnp.sum(faces[...], axis=0)

    def dot(left, right):
        return jnp.dot(left, right, precision=highest, preferred_element_type=jnp.float32)

    cell = iota((128, depth), 0)
    fine = iota((128, depth), 1)
    expand = []
    for i in range(3):
        place = cell - plan.marks[i]
        table = weights(fine, place + plan.start_z(me_z))
        expand.append(jnp.where((place >= 0) & (place < reach_z), table, 0.0))
    shape = (cols, plan.rows)
    cell = iota(shape, 1)
    table = weights(iota(shape, 0) + at_y, cell + plan.start(1, me_y))
    inner_y = jnp.where(cell < reach_y, table, 0.0)
    shape = (rows, plan.rows)
    cell = iota(shape, 1)
    inner_x = []
    for e in range(2):
        place = cell - e * reach_x
        table = weights(iota(shape, 0) + at_x, place + plan.start(0, me_x))
        inner_x.append(jnp.where((place >= 0) & (place < reach_x), table, 0.0))
    cell = iota((128, 128), 0) - plan.marks[3]
    fine = iota((128, 128), 1)
    edge_x = []
    for e in range(2):
        table = weights(fine + at_x, (cell >> 1) + plan.start(0, me_x))
        edge_x.append(jnp.where((cell >= 0) & (cell < 2 * reach_x) & ((cell & 1) == e), table, 0.0))

    ghost_x = [dot(inner_y, dot(face, expand[e])) for e in range(2)]
    lines = dot(face, expand[2])
    ghost_y = [dot(inner_x[e], lines) for e in range(2)]
    column = dot(inner_y, face)
    ghost_z = [dot(column, edge_x[e]) for e in range(2)]

    y = iota((cols, depth), 0) + at_y
    z = iota((cols, depth), 1)
    scale = jnp.where((y >= 0) & (y < total_y), 1.0 / 6.0, 0.0)

    def whole(index, x):
        mine, theirs = own[index, x], other[index, x]
        left = jnp.where(me_z == 0, mine, theirs)
        right = jnp.where(me_z == 0, theirs, mine)
        return jnp.concatenate([left, right], axis=1)

    for x in range(rows):
        here = at_x + x
        value = whole(0, x) * (-1.0 / (RATIO * RATIO))
        value += jnp.where(here == 0, ghost_x[0], 0.0) + jnp.where(here == total_x - 1, ghost_x[1], 0.0)
        value += jnp.where(y == 0, ghost_y[0][x : x + 1], 0.0)
        value += jnp.where(y == total_y - 1, ghost_y[1][x : x + 1], 0.0)
        value += jnp.where(z == 0, ghost_z[0][:, x : x + 1], 0.0)
        value += jnp.where(z == total_z - 1, ghost_z[1][:, x : x + 1], 0.0)
        source[x] = value
        values[0, x] = whole(1, x)

    for sweep in range(width):
        now, later = sweep % 2, (sweep + 1) % 2
        margin = sweep + 1

        for x in range(margin, rows - margin):
            here = at_x + x
            value = values[now, x]
            total = values[now, x - 1] + values[now, x + 1]
            total += pltpu.roll(value, 1, 0) + pltpu.roll(value, cols - 1, 0)
            total += jnp.where(z == 0, 0.0, pltpu.roll(value, 1, 1))
            total += jnp.where(z == depth - 1, 0.0, pltpu.roll(value, depth - 1, 1))
            keep = jnp.where((here >= 0) & (here < total_x), 1.0, 0.0)
            values[later, x] = (total + source[x]) * (scale * keep)

    for x in range(plan.fine[0]):
        value = values[width % 2, width + x, width : cols - width]
        half = plan.fine[2]
        out[x] = jnp.where(me_z == 0, value[:, :half], value[:, half:])


def step_of(coarse_density, fine_density, fine_start, anchor):
    fine = fine_start.shape
    counts = tuple(lax.axis_size(axis) for axis in ("gx", "gy", "grp"))
    plan = Plan(fine, counts)
    width = SWEEPS
    both = jnp.stack([fine_density, fine_start])
    both = with_halo(both, "gx", 1, width)
    both = with_halo(both, "gy", 2, width)
    other = lax.ppermute(both, "grp", [(0, 1), (1, 0)])

    potential = coarse_solve(coarse_density)
    faces = box_faces(plan, potential, anchor)
    faces = lax.all_to_all(faces, EVERY, split_axis=0, concat_axis=0, tiled=True)
    padded = (fine[0] + 2 * width, fine[1] + 2 * width, 2 * fine[2])
    values = pl.pallas_call(
        functools.partial(sweep_kernel, plan, width),
        out_shape=jax.ShapeDtypeStruct(fine, jnp.float32),
        in_specs=[pl.BlockSpec(memory_space=pltpu.VMEM)] * 3,
        out_specs=pl.BlockSpec(memory_space=pltpu.VMEM),
        scratch_shapes=[pltpu.VMEM(padded, jnp.float32), pltpu.VMEM((2,) + padded, jnp.float32)],
        compiler_params=pltpu.CompilerParams(vmem_limit_bytes=VMEM_LIMIT),
        name="sweeps",
    )(faces, both, other)
    return (potential, values)


def solution(mesh):
    return jax.shard_map(
        step_of,
        mesh=mesh,
        in_specs=(P("gx", ("grp", "gy"), None), P("gx", "gy", "grp"), P("gx", "gy", "grp"), P()),
        out_specs=(P("gx", ("grp", "gy"), None), P("gx", "gy", "grp")),
        check_vma=False,
    )
```

```python
import functools
import math

import jax
import jax.numpy as jnp
import numpy as np
from jax import lax
from jax.experimental import pallas as pl
from jax.experimental.pallas import tpu as pltpu
from jax.sharding import PartitionSpec as P


RATIO = 4
SWEEPS = 8
EVERY = ("gx", "grp", "gy")
VMEM_LIMIT = 50 * 1024 * 1024
WIDE_LIMIT = 60 * 1024 * 1024
SMALL_LIMIT = 20 * 1024 * 1024
AHEAD = 8

highest = lax.Precision.HIGHEST


def with_halo(block, axis, dim, width):
    count = lax.axis_size(axis)
    forward = [(i, i + 1) for i in range(count - 1)]
    backward = [(target, source) for source, target in forward]
    low = lax.ppermute(
        lax.slice_in_dim(block, block.shape[dim] - width, None, axis=dim), axis, forward
    )
    high = lax.ppermute(lax.slice_in_dim(block, 0, width, axis=dim), axis, backward)
    return jnp.concatenate([low, block, high], axis=dim)


def sine_table(amount):
    indices = np.arange(1, amount + 1, dtype=np.int64)
    product = indices[:, None] * indices[None, :] % (2 * (amount + 1))
    return math.sqrt(2.0 / (amount + 1)) * np.sin(product * (math.pi / (amount + 1)))


def eigen_values(amount):
    return -4.0 * np.square(np.sin(np.arange(1, amount + 1) * (math.pi / (2 * (amount + 1)))))


def parity_order(amount):
    return np.concatenate([np.arange(0, amount, 2), np.arange(1, amount, 2)])


def halves(table):
    top = table.astype(np.float32).astype(jnp.bfloat16)
    rest = (table - top.astype(np.float64)).astype(np.float32).astype(jnp.bfloat16)
    return top, rest


def folded_tables(amount):
    table = sine_table(amount)[: amount // 2]
    even, odd = table[:, 0::2], table[:, 1::2]
    forward, inverse = [], []
    for part in (even, odd):
        top, rest = halves(part)
        forward.append(np.concatenate([top, top, rest], axis=0))
        top, rest = halves(part.T)
        inverse.append(np.concatenate([top, top, rest], axis=0))
    return np.stack(forward), np.stack(inverse)


def decay_table(cols, depth):
    lam_z = eigen_values(depth)[parity_order(depth)]
    size = -(eigen_values(cols)[:, None] + lam_z[None, :])
    return (2.0 / (2.0 + size + np.sqrt(size * (size + 4.0)))).astype(np.float32)


def split(values):
    top = values.astype(jnp.bfloat16)
    return top, (values - top.astype(jnp.float32)).astype(jnp.bfloat16)


def reverse_lanes(values):
    rows, width = values.shape
    tiles = width // 128
    index = 127 - lax.broadcasted_iota(jnp.int32, (rows, 128), 1)
    parts = [
        jnp.take_along_axis(values[:, t * 128 : (t + 1) * 128], index, axis=1)
        for t in reversed(range(tiles))
    ]
    return jnp.concatenate(parts, axis=1)


def dot32(left, right):
    return jnp.dot(left, right, preferred_element_type=jnp.float32)


def triple(values):
    top, rest = split(values)
    return jnp.concatenate([top, rest, top], axis=1)


def cols_transform(sine3, values):
    top, rest = split(values)
    return dot32(sine3, jnp.concatenate([top, rest, top], axis=0))


def forward_kernel(shape, chunk, block, depth_table, sine3, sine, decay, ends, out_w, *rest):
    rows, cols, depth = shape
    half = depth // 2
    count = rows // chunk
    step = pl.program_id(0)
    *out_t, w, traces, sems, loads = rest

    def send(index):
        part = pl.ds(index * chunk, chunk)
        return pltpu.make_async_copy(w.at[part], out_w.at[part], sems.at[index])

    def load(index):
        part = pl.ds(index * chunk, chunk)
        return pltpu.make_async_copy(block.at[part], w.at[part], loads.at[index])

    @pl.when(step == 0)
    def _():
        for index in range(min(AHEAD, count)):
            load(index).start()

    load(step).wait()

    @pl.when(step + AHEAD < count)
    def _():
        load(step + AHEAD).start()

    values = w[pl.ds(step * chunk, chunk)].reshape(chunk * cols, depth)
    low = values[:, :half]
    high = reverse_lanes(values[:, half:])
    even = dot32(triple(low + high), depth_table[0])
    odd = dot32(triple(low - high), depth_table[1])
    even = even.reshape(chunk, cols, half)
    odd = odd.reshape(chunk, cols, half)
    rate = decay[...]
    for x in range(chunk):
        here = step * chunk + x
        now = cols_transform(sine3[...], jnp.concatenate([even[x], odd[x]], axis=1))
        if x == 0:
            before = w[jnp.maximum(here - 1, 0)]
            before = jnp.where(step == 0, 0.0, before)
        else:
            before = w[here - 1]
        w[here] = rate * (before - now)

    @pl.when(step > 0)
    def _():
        send(step - 1).start()

    @pl.when(step == count - 1)
    def _():
        send(step).start()
        for tile in range(depth // 128):
            lanes = slice(tile * 128, (tile + 1) * 128)
            rate = decay[:, lanes]
            first = ends[:, 0:1] * jnp.ones((1, 128), jnp.float32)
            sign = 1.0 - 2.0 * (lax.broadcasted_iota(jnp.int32, (8, 128), 0) % 2).astype(jnp.float32)

            def back(i, value):
                base = pl.multiple_of((rows // 8 - 1 - i) * 8, 8)
                got_first, got_second = [None] * 8, [None] * 8
                for x in reversed(range(8)):
                    value = w[base + x, :, lanes] + rate * value
                    partial = jnp.sum((value * first).reshape(cols // 8, 8, 128), axis=0)
                    got_first[x] = jnp.sum(partial, axis=0, keepdims=True)
                    got_second[x] = jnp.sum(partial * sign, axis=0, keepdims=True)
                traces[pl.ds(base, 8), lanes] = jnp.concatenate(got_first, axis=0)
                traces[pl.ds(rows + base, 8), lanes] = jnp.concatenate(got_second, axis=0)
                return value

            start = lax.fori_loop(0, rows // 8, back, jnp.zeros((cols, 128), jnp.float32))
            for index, plane in enumerate((start, w[rows - 1, :, lanes])):
                top = 2 * rows + index * cols
                traces[top : top + cols, lanes] = jnp.dot(
                    sine[...], plane, precision=highest, preferred_element_type=jnp.float32
                )
        size = depth // len(out_t)
        for index, target in enumerate(out_t):
            target[...] = traces[:, index * size : (index + 1) * size].T
        for index in range(count):
            send(index).wait()


def inverse_kernel(shape, chunk, parts, swept, *rest):
    rows, cols, depth = shape
    half = depth // 2
    count = rows // chunk
    step = pl.program_id(0)
    back, rest = rest[:parts], rest[parts:]
    depth_table, sine3, sine, decay, ends, out, w, known, carry, sems, loads = rest

    def load(index):
        part = pl.ds(index * chunk, chunk)
        return pltpu.make_async_copy(swept.at[part], w.at[part], loads.at[index])

    def send(index):
        part = pl.ds(index * chunk, chunk)
        return pltpu.make_async_copy(w.at[part], out.at[part], sems.at[index])

    @pl.when(step == 0)
    def _():
        for index in range(min(AHEAD, count)):
            load(index).start()
        size = depth // parts
        for index in range(parts):
            known[:, index * size : (index + 1) * size] = back[index][...].T
        planes = [
            jnp.dot(
                sine[...],
                known[2 * rows + index * cols : 2 * rows + (index + 1) * cols],
                precision=highest,
                preferred_element_type=jnp.float32,
            )
            for index in range(2)
        ]
        carry[0] = planes[0]
        carry[1] = planes[1]

    @pl.when(step < count)
    def _():
        rate = decay[...]
        first = ends[:, 0:1] * jnp.ones((1, depth), jnp.float32)
        even = lax.broadcasted_iota(jnp.int32, (8, depth), 0) % 2 == 0
        value = carry[0]
        load(step).wait()

        @pl.when(step + AHEAD < count)
        def _():
            load(step + AHEAD).start()

        for x in range(chunk):
            here = step * chunk + x
            low, high = known[pl.ds(here, 1)], known[pl.ds(rows + here, 1)]
            both = jnp.where(even, low + high, low - high)
            both = jnp.concatenate([both] * (cols // 8), axis=0)
            value = rate * (value + first * both)
            w[here] = w[here] + value
        carry[0] = value

    @pl.when(step == count - 1)
    def _():
        w[rows - 1] = w[rows - 1] + decay[...] * carry[1]
        carry[0] = jnp.zeros((cols, depth), jnp.float32)

    @pl.when(step >= count)
    def _():
        place = 2 * count - 1 - step
        base = place * chunk
        rate = decay[...]
        value = carry[0]
        planes = [None] * chunk
        for x in reversed(range(chunk)):
            value = w[base + x] + rate * value
            planes[x] = cols_transform(sine3[...], value)
        carry[0] = value
        values = jnp.concatenate(planes, axis=0)
        even = dot32(triple(values[:, :half]), depth_table[0])
        odd = dot32(triple(values[:, half:]), depth_table[1])
        result = jnp.concatenate([even + odd, reverse_lanes(even - odd)], axis=1)
        w[pl.ds(base, chunk)] = result.reshape(chunk, cols, depth)

        @pl.when(step > count)
        def _():
            send(place + 1).start()

        @pl.when(step == 2 * count - 1)
        def _():
            send(place).start()
            for index in range(count):
                send(index).wait()


def local_tables(shape):
    _, cols, depth = shape
    forward, inverse = folded_tables(depth)
    sine = sine_table(cols)
    top, rest = halves(sine)
    sine3 = np.concatenate([top, top, rest], axis=1)
    ends = np.stack([sine[:, 0], sine[:, -1]], axis=1).astype(np.float32)
    return forward, inverse, (sine3, sine.astype(np.float32), decay_table(cols, depth), ends)


def full(array):
    return pl.BlockSpec(array.shape, lambda i, rank=array.ndim: (0,) * rank)


def coarse_solve(density):
    rows, cols, depth = density.shape
    shape = density.shape
    strips = lax.axis_size("gx")
    bands = lax.axis_size(("grp", "gy"))
    devices = strips * bands
    parts = 2 if depth % (16 * devices) == 0 else 1
    share = depth // (devices * parts)
    chunk = 16
    count = rows // chunk
    width = 2 * cols + 2 * rows
    forward, inverse, tables = local_tables(shape)
    params, wide = (
        pltpu.CompilerParams(dimension_semantics=("arbitrary",), vmem_limit_bytes=limit)
        for limit in (VMEM_LIMIT, WIDE_LIMIT)
    )
    swept, *traces = pl.pallas_call(
        functools.partial(forward_kernel, shape, chunk),
        grid=(count,),
        in_specs=[pl.BlockSpec(memory_space=pl.ANY), full(forward)]
        + [full(table) for table in tables],
        out_specs=[pl.BlockSpec(memory_space=pl.ANY)]
        + [pl.BlockSpec((depth // parts, width), lambda i: (0, 0))] * parts,
        out_shape=[jax.ShapeDtypeStruct(shape, jnp.float32)]
        + [jax.ShapeDtypeStruct((depth // parts, width), jnp.float32)] * parts,
        scratch_shapes=[
            pltpu.VMEM(shape, jnp.float32),
            pltpu.VMEM((width, depth), jnp.float32),
            pltpu.SemaphoreType.DMA((count,)),
            pltpu.SemaphoreType.DMA((count,)),
        ],
        compiler_params=wide,
        cost_estimate=cost(30e9),
        name="local_forward",
    )(density, forward, *tables)

    back = []
    for index in range(parts):
        packed = lax.all_to_all(
            traces[index].reshape(devices, share, width), EVERY, split_axis=0, concat_axis=0, tiled=True
        )
        sides = middle(packed, rows, cols, strips, bands, depth, index * devices * share)
        sides = lax.all_to_all(sides, EVERY, split_axis=0, concat_axis=0, tiled=True)
        back.append(sides.reshape(depth // parts, width))

    return pl.pallas_call(
        functools.partial(inverse_kernel, shape, chunk, parts),
        grid=(2 * count,),
        in_specs=[
            pl.BlockSpec(memory_space=pl.ANY),
            *[full(part) for part in back],
            full(inverse),
        ]
        + [full(table) for table in tables],
        out_specs=pl.BlockSpec(memory_space=pl.ANY),
        out_shape=jax.ShapeDtypeStruct(shape, jnp.float32),
        scratch_shapes=[
            pltpu.VMEM(shape, jnp.float32),
            pltpu.VMEM((width, depth), jnp.float32),
            pltpu.VMEM((2, cols, depth), jnp.float32),
            pltpu.SemaphoreType.DMA((count,)),
            pltpu.SemaphoreType.DMA((count,)),
        ],
        compiler_params=params,
        cost_estimate=cost(30e9),
        name="local_inverse",
    )(swept, *back, inverse, *tables)


def thirds(values):
    first = values.astype(jnp.bfloat16).astype(jnp.float32)
    rest = values - first
    second = rest.astype(jnp.bfloat16).astype(jnp.float32)
    return first, second, rest - second


def middle_tables(rows, cols, strips, bands, share):
    count_0, count_1 = 2 * strips, 2 * bands
    table_0, table_1 = sine_table(rows * strips), sine_table(cols * bands)

    def stacked(table):
        top, rest = halves(table)
        return np.concatenate([top, top, rest], axis=0)

    def ends(table, count, size):
        picked = table.reshape(count, size, -1)[:, [0, size - 1]].reshape(2 * count, -1)
        return picked.astype(np.float32), np.concatenate(halves(picked), axis=0)

    def shuffle(count, swap):
        matrix = np.zeros((count * share, count * share), np.float32)
        for plane in range(count):
            other = plane if not swap else ((plane - 1) ^ 1) + 1
            if 0 <= other < count:
                for k in range(share):
                    matrix[k * count + plane, other * share + k] = 1.0
        return matrix

    blocks = np.kron(np.eye(128 // cols), sine_table(cols))
    gather_0 = shuffle(count_0, False).astype(jnp.bfloat16)
    gather_1 = -shuffle(count_1, True)
    scatter_1 = -gather_1.T
    tables = [stacked(table_0)]
    if rows * strips != cols * bands:
        tables.append(stacked(table_1))
    return (
        *tables,
        stacked(blocks),
        *ends(table_0, strips, rows),
        *ends(table_1, bands, cols),
        gather_0,
        np.ascontiguousarray(gather_0.T),
        gather_1.astype(jnp.bfloat16),
        np.ascontiguousarray(scatter_1).astype(jnp.bfloat16),
        eigen_values(rows * strips).astype(np.float32)[:, None],
        eigen_values(cols * bands).astype(np.float32)[None, :],
        np.tile(eigen_values(cols), bands).astype(np.float32)[None, :],
    )


def middle_kernel(
    sizes, block, packed, lam_own, full_0, *more,
):
    full_1, more = (full_0, more) if sizes[0] * sizes[2] == sizes[1] * sizes[3] else (more[0], more[1:])
    interfaces(sizes, block, packed, lam_own, full_0, full_1, *more)


def interfaces(
    sizes, block, packed, lam_own, full_0, full_1, blocks, sides_0, stack_0, sides_1, stack_1,
    gather_0, scatter_0, gather_1, scatter_1, lam_0, lam_1, lam_y, out, source_0, source_1, wave_0, wave_1, planes_0, planes_1,
):
    rows, cols, strips, bands, share = sizes
    count_0, count_1 = 2 * strips, 2 * bands
    step = pl.program_id(0)

    def swapped(plane, count):
        other = ((plane - 1) ^ 1) + 1
        return other if 0 <= other < count else None

    def scaled(values):
        size = -(lam_y[...] + lam_own[...])
        rate = 2.0 / (2.0 + size + jnp.sqrt(size * (size + 4.0)))
        rate = jnp.concatenate([rate] * strips, axis=0)
        result = []
        for start in range(0, lam_y.shape[1], 128):
            part = slice(start, start + 128)
            value = dot32(triple(values[:, part]), blocks[...]) * rate[:, part]
            result.append(dot32(triple(value), blocks[...]))
        return jnp.concatenate(result, axis=1)

    def line(values, plane):
        return values[plane * share : (plane + 1) * share]

    @pl.when(step == 0)
    def _():
        for b in range(bands):
            for e in range(2):
                lanes = slice(e * rows, (e + 1) * rows)
                parts = [packed[s * bands + b, :, lanes] for s in range(strips)]
                plane = 2 * b + e
                planes_1[plane * share : (plane + 1) * share] = jnp.concatenate(parts, axis=1)
        for s in range(strips):
            for e in range(2):
                lanes = slice(2 * rows + e * cols, 2 * rows + (e + 1) * cols)
                parts = [packed[s * bands + b, :, lanes] for b in range(bands)]
                plane = 2 * s + e
                planes_0[plane * share : (plane + 1) * share] = jnp.concatenate(parts, axis=1)
        value = planes_0[...]
        own = scaled(jnp.concatenate([line(value, 2 * s) for s in range(strips)], axis=0))
        parts = []
        for plane in range(count_0):
            part = jnp.zeros_like(line(value, 0))
            other = swapped(plane, count_0)
            if other is not None:
                part = part - line(value, other)
            if plane % 2 == 0:
                part = part + line(own, plane // 2)
            parts.append(part)
        value = exact_dot(gather_0[...], jnp.concatenate(parts, axis=0))
        source_0[...] = dot32(triple(value), full_1[...]).reshape(source_0.shape)
        value = exact_dot(gather_1[...], planes_1[...])
        source_1[...] = dot32(triple(value), full_0[...]).reshape(source_1.shape)

    left = jnp.concatenate([sides_0[...], source_1[step]], axis=0)
    right = jnp.concatenate([source_0[step], sides_1[...]], axis=0)
    a1, a2 = split(left)
    b1, b2 = split(right)
    a1, a2 = a1.astype(jnp.float32), a2.astype(jnp.float32)
    left = jnp.concatenate([a1, a1, a2], axis=0)
    right = jnp.concatenate([b1.astype(jnp.float32), b2.astype(jnp.float32), b1.astype(jnp.float32)], axis=0)
    right = right.astype(jnp.bfloat16)
    offset = lam_1[...] + lam_own[pl.ds(step, 1)]
    total = jnp.zeros((2 * count_0, lam_1.shape[1]), jnp.float32)
    dims = (((1,), (1,)), ((), ()))
    for start in range(0, lam_0.shape[0], block):
        part = slice(start, start + block)
        wave = dot32(left[:, part].T.astype(jnp.bfloat16), right) / (lam_0[part] + offset)
        top, rest = split(wave)
        total += dot32(stack_0[:, part], top) + dot32(stack_0[:, part], rest)
        other = lax.dot_general(stack_1[...], top, dims, preferred_element_type=jnp.float32)
        other += lax.dot_general(stack_1[...], rest, dims, preferred_element_type=jnp.float32)
        wave_1[step, :, part] = other[:count_1] + other[count_1:]
    wave_0[step] = total[:count_0] + total[count_0:]

    @pl.when(step == share - 1)
    def _():
        value = dot32(triple(wave_0[...].reshape(share * count_0, -1)), full_1[...])
        value = planes_0[...] + exact_dot(scatter_0[...], value)
        own = scaled(jnp.concatenate([line(value, 2 * s) for s in range(strips)], axis=0))
        edge_0 = []
        for plane in range(count_0):
            part = jnp.zeros_like(line(value, 0))
            other = swapped(plane, count_0)
            if other is not None:
                part = part + line(value, other)
            if plane % 2 == 0:
                part = part - line(own, plane // 2)
            edge_0.append(part)
        value = dot32(triple(wave_1[...].reshape(share * count_1, -1)), full_0[...])
        value = exact_dot(scatter_1[...], value)
        edge_1 = []
        for plane in range(count_1):
            part = line(value, plane)
            other = swapped(plane, count_1)
            if other is not None:
                part = part + planes_1[other * share : (other + 1) * share]
            edge_1.append(part)
        for s in range(strips):
            for b in range(bands):
                parts = [edge_1[2 * b + e][:, s * rows : (s + 1) * rows] for e in range(2)]
                parts += [edge_0[2 * s + e][:, b * cols : (b + 1) * cols] for e in range(2)]
                out[s * bands + b] = jnp.concatenate(parts, axis=1)


def middle(packed, rows, cols, strips, bands, depth, offset):
    _, share, _ = packed.shape
    sizes = (rows, cols, strips, bands, share)
    lam = jnp.asarray(eigen_values(depth)[parity_order(depth)].astype(np.float32))
    lam = lax.dynamic_slice(lam, (offset + lax.axis_index(EVERY) * share,), (share,))
    tables = middle_tables(*sizes)
    length_0, length_1 = rows * strips, cols * bands
    return pl.pallas_call(
        functools.partial(middle_kernel, sizes, math.gcd(512, length_0)),
        grid=(share,),
        in_specs=[
            full(packed),
            pl.BlockSpec((share, 1), lambda i: (0, 0)),
        ]
        + [full(table) for table in tables],
        out_specs=pl.BlockSpec(packed.shape, lambda i: (0, 0, 0)),
        out_shape=jax.ShapeDtypeStruct(packed.shape, jnp.float32),
        scratch_shapes=[
            pltpu.VMEM((share, 2 * strips, length_1), jnp.float32),
            pltpu.VMEM((share, 2 * bands, length_0), jnp.float32),
            pltpu.VMEM((share, 2 * strips, length_1), jnp.float32),
            pltpu.VMEM((share, 2 * bands, length_0), jnp.float32),
            pltpu.VMEM((2 * strips * share, length_1), jnp.float32),
            pltpu.VMEM((2 * bands * share, length_0), jnp.float32),
        ],
        compiler_params=pltpu.CompilerParams(
            dimension_semantics=("arbitrary",), vmem_limit_bytes=SMALL_LIMIT
        ),
        cost_estimate=cost(20e9),
        name="interfaces",
    )(packed, lam.reshape(share, 1), *tables)


def cost(flops):
    return pl.CostEstimate(flops=int(flops), bytes_accessed=1 << 24, transcendentals=0)


def weights(fine_index, cell):
    scaled = 2 * fine_index + 1 + RATIO
    bottom = scaled >> 3
    weight = (scaled & 7).astype(jnp.float32) * 0.125
    return jnp.where(cell == bottom, 1.0 - weight, jnp.where(cell == bottom + 1, weight, 0.0))


def end_weights(total):
    result = []
    for index in (-1, total):
        scaled = 2 * index + 1 + RATIO
        result.append((scaled // (2 * RATIO), (scaled % (2 * RATIO)) / (2.0 * RATIO)))
    return result


class Plan:
    def __init__(self, fine, counts):
        self.fine = fine
        self.counts = counts
        self.totals = tuple(size * count for size, count in zip(fine, counts))
        self.bounds = tuple(total // RATIO + 2 for total in self.totals)
        self.reach = [size // RATIO + 6 for size in fine]
        if counts[2] == 2:
            self.reach[2] -= 2
        assert self.reach[0] <= 8 and self.reach[1] <= 16 and min(counts[:2]) > 2
        self.rows = 16
        self.marks = tuple(self.reach[2] * i for i in range(4))

    def end(self, dim, index):
        return int(2 * index >= self.counts[dim])

    def edge(self, dim, index):
        return jnp.where(2 * index >= self.counts[dim], self.totals[dim] - 1, 0)

    def start(self, dim, index):
        return index * (self.fine[dim] // RATIO) - 2

    def start_z(self, index):
        first = self.start(2, index)
        last = self.bounds[2] - self.reach[2]
        if isinstance(index, int):
            return min(max(first, 0), last)
        return jnp.clip(first, 0, last)


def iota(shape, dim):
    return lax.broadcasted_iota(jnp.int32, shape, dim)


def exact_dot(left, right):
    return sum(dot32(left, part.astype(jnp.bfloat16)) for part in thirds(right))


def faces_kernel(plan, shape, near, anchor, potential, out, slab, plane, sem):
    rows, cols, depth = shape
    bound_x, bound_y, bound_z = plan.bounds
    reach_x, reach_y, _ = plan.reach
    count_x, count_y, count_z = plan.counts
    shift_x = anchor[0] - 1 - lax.axis_index("gx") * rows
    band = lax.axis_index("grp") * count_y + lax.axis_index("gy")
    shift_y = anchor[1] - 1 - band * cols
    base_z = anchor[2] - 1
    from_x = jnp.clip(shift_x, 0, rows - near)
    copy = pltpu.make_async_copy(potential.at[pl.ds(from_x, near)], slab, sem)
    copy.start()

    parts = []
    cell = iota((depth, 128), 0) - base_z
    lane = iota((depth, 128), 1)
    ends_z = end_weights(plan.totals[2])
    last = (lane >= plan.marks[3]) & (lane < plan.marks[3] + 2 * reach_x)
    for g in range(count_z):
        want = jnp.full((depth, 128), -1, jnp.int32)
        for i in range(3):
            inside = (lane >= plan.marks[i]) & (lane < plan.marks[i + 1])
            want = jnp.where(inside, lane - plan.marks[i] + plan.start_z(g), want)
        hit = (want >= 0) & (want < bound_z) & (cell == want)
        bottom, weight = ends_z[plan.end(2, g)]
        edge = jnp.where(cell == bottom, 1.0 - weight, jnp.where(cell == bottom + 1, weight, 0.0))
        edge = jnp.where(last, edge, 0.0)
        parts.append(jnp.where(hit, 1.0, edge).astype(jnp.bfloat16))
    select_z = jnp.concatenate(parts, axis=1)

    high = count_y * plan.rows
    cell = iota((high, cols), 1) - shift_y
    row = iota((high, cols), 0)
    want = (row // plan.rows) * (plan.fine[1] // RATIO) - 2 + row % plan.rows
    ok = (want >= 0) & (want < bound_y) & (row % plan.rows < reach_y) & (cell == want)
    select_y = jnp.where(ok, 1.0, 0.0)
    cell = iota((plan.rows, cols), 1) - shift_y
    row = iota((plan.rows, cols), 0)
    edge = jnp.zeros((plan.rows, cols), jnp.float32)
    for e, (bottom, weight) in enumerate(end_weights(plan.totals[1])):
        here = jnp.where(cell == bottom, 1.0 - weight, jnp.where(cell == bottom + 1, weight, 0.0))
        edge = jnp.where((row >= e * reach_x) & (row < (e + 1) * reach_x), here, edge)
    select_y = jnp.concatenate([select_y, edge], axis=0).astype(jnp.bfloat16)

    copy.wait()
    for x in range(near):
        line = sum(dot32(part.astype(jnp.bfloat16), select_z) for part in thirds(slab[x]))
        plane[x] = exact_dot(select_y, line)

    cells = []
    for a in range(bound_x):
        place = shift_x + a - from_x
        ok = (place >= 0) & (place < near)
        got = plane[jnp.clip(place, 0, near - 1)]
        cells.append(jnp.where(ok, got, 0.0))
    ends = []
    for bottom, weight in end_weights(plan.totals[0]):
        ends.append((1.0 - weight) * cells[bottom] + weight * cells[bottom + 1])

    lane = iota((8, 128), 1)
    row = iota((8, 128), 0)
    for dx in range(count_x):
        first = plan.start(0, dx)
        inside = [t for t in range(reach_x) if 0 <= first + t < bound_x]
        face_x = ends[plan.end(0, dx)]
        for g in range(count_z):
            lanes = slice(g * 128, (g + 1) * 128)
            face_y = [jnp.zeros((8, 128), jnp.float32)] * 2
            for e in range(2):
                top = high + e * reach_x
                for t in inside:
                    face_y[e] = jnp.where(row == t, cells[first + t][top : top + 8, lanes], face_y[e])
            for dy in range(count_y):
                parts = [slice(dy * plan.rows + 8 * h, dy * plan.rows + 8 * h + 8) for h in range(2)]
                value = jnp.where(lane < plan.marks[3], face_y[plan.end(1, dy)], 0.0)
                for t in inside:
                    for h in range(2):
                        here = lane == plan.marks[3] + 2 * t + h
                        value = jnp.where(here, cells[first + t][parts[h], lanes], value)
                value = jnp.where(lane < plan.marks[2], face_x[parts[1], lanes], value)
                value = jnp.where(lane < plan.marks[1], face_x[parts[0], lanes], value)
                out[(dx * count_z + g) * count_y + dy] = value


def box_faces(plan, potential, anchor):
    shape = potential.shape
    near = min(plan.bounds[0], shape[0])
    devices = math.prod(plan.counts)
    return pl.pallas_call(
        functools.partial(faces_kernel, plan, shape, near),
        in_specs=[pl.BlockSpec(memory_space=pltpu.SMEM), pl.BlockSpec(memory_space=pl.ANY)],
        out_specs=pl.BlockSpec(memory_space=pltpu.VMEM),
        out_shape=jax.ShapeDtypeStruct((devices, 8, 128), jnp.float32),
        scratch_shapes=[
            pltpu.VMEM((near,) + shape[1:], jnp.float32),
            pltpu.VMEM((near, (plan.counts[1] + 1) * plan.rows, plan.counts[2] * 128), jnp.float32),
            pltpu.SemaphoreType.DMA,
        ],
        compiler_params=pltpu.CompilerParams(vmem_limit_bytes=VMEM_LIMIT),
        name="faces",
    )(anchor, potential)


def sweep_kernel(plan, width, faces, own, other, out, source, values):
    rows, cols, depth = (size + 2 * width for size in plan.fine)
    depth = 2 * plan.fine[2]
    reach_x, reach_y, reach_z = plan.reach
    total_x, total_y, _ = plan.totals
    me_x, me_y, me_z = (lax.axis_index(axis) for axis in ("gx", "gy", "grp"))
    at_x = me_x * plan.fine[0] - width
    at_y = me_y * plan.fine[1] - width
    face = jnp.sum(faces[...], axis=0)

    def dot(left, right):
        return jnp.dot(left, right, precision=highest, preferred_element_type=jnp.float32)

    cell = iota((128, depth), 0)
    fine = iota((128, depth), 1)
    expand = []
    for i in range(3):
        place = cell - plan.marks[i]
        table = weights(fine, place + plan.start_z(me_z))
        expand.append(jnp.where((place >= 0) & (place < reach_z), table, 0.0))
    shape = (cols, 8)
    inner_y = []
    for h in range(2):
        cell = iota(shape, 1) + 8 * h
        table = weights(iota(shape, 0) + at_y, cell + plan.start(1, me_y))
        inner_y.append(jnp.where(cell < reach_y, table, 0.0))
    cell = iota((rows, 8), 1)
    table = weights(iota((rows, 8), 0) + at_x, cell + plan.start(0, me_x))
    inner_x = jnp.where(cell < reach_x, table, 0.0)
    cell = iota((128, 128), 0) - plan.marks[3]
    table = weights(iota((128, 128), 1) + at_x, (cell >> 1) + plan.start(0, me_x))
    ok = (cell >= 0) & (cell < 2 * reach_x)
    edge_x = [jnp.where(ok & ((cell & 1) == h), table, 0.0) for h in range(2)]

    ghost_x = sum(dot(inner_y[h], dot(face, expand[h])) for h in range(2))
    ghost_y = dot(inner_x, dot(face, expand[2]))
    ghost_z = sum(dot(inner_y[h], dot(face, edge_x[h])) for h in range(2))
    edges = [plan.edge(dim, index) for dim, index in enumerate((me_x, me_y, me_z))]

    y = iota((cols, depth), 0) + at_y
    z = iota((cols, depth), 1)
    scale = jnp.where((y >= 0) & (y < total_y), 1.0 / 6.0, 0.0)

    def whole(index, x):
        mine, theirs = own[index, x], other[index, x]
        left = jnp.where(me_z == 0, mine, theirs)
        right = jnp.where(me_z == 0, theirs, mine)
        return jnp.concatenate([left, right], axis=1)

    for x in range(rows):
        here = at_x + x
        value = whole(0, x) * (-1.0 / (RATIO * RATIO))
        value += jnp.where(here == edges[0], ghost_x, 0.0)
        value += jnp.where(y == edges[1], ghost_y[x : x + 1], 0.0)
        value += jnp.where(z == edges[2], ghost_z[:, x : x + 1], 0.0)
        source[x] = value
        values[0, x] = whole(1, x)

    for sweep in range(width):
        now, later = sweep % 2, (sweep + 1) % 2
        margin = sweep + 1

        for x in range(margin, rows - margin):
            here = at_x + x
            value = values[now, x]
            total = values[now, x - 1] + values[now, x + 1]
            total += pltpu.roll(value, 1, 0) + pltpu.roll(value, cols - 1, 0)
            total += jnp.where(z == 0, 0.0, pltpu.roll(value, 1, 1))
            total += jnp.where(z == depth - 1, 0.0, pltpu.roll(value, depth - 1, 1))
            keep = jnp.where((here >= 0) & (here < total_x), 1.0, 0.0)
            values[later, x] = (total + source[x]) * (scale * keep)

    for x in range(plan.fine[0]):
        value = values[width % 2, width + x, width : cols - width]
        half = plan.fine[2]
        out[x] = jnp.where(me_z == 0, value[:, :half], value[:, half:])


def step_of(coarse_density, fine_density, fine_start, anchor):
    fine = fine_start.shape
    counts = tuple(lax.axis_size(axis) for axis in ("gx", "gy", "grp"))
    plan = Plan(fine, counts)
    width = SWEEPS
    both = jnp.stack([fine_density, fine_start])
    both = with_halo(both, "gx", 1, width)
    both = with_halo(both, "gy", 2, width)
    other = lax.ppermute(both, "grp", [(0, 1), (1, 0)])

    potential = coarse_solve(coarse_density)
    faces = box_faces(plan, potential, anchor)
    faces = lax.all_to_all(faces, EVERY, split_axis=0, concat_axis=0, tiled=True)
    padded = (fine[0] + 2 * width, fine[1] + 2 * width, 2 * fine[2])
    values = pl.pallas_call(
        functools.partial(sweep_kernel, plan, width),
        out_shape=jax.ShapeDtypeStruct(fine, jnp.float32),
        in_specs=[pl.BlockSpec(memory_space=pltpu.VMEM)] * 3,
        out_specs=pl.BlockSpec(memory_space=pltpu.VMEM),
        scratch_shapes=[pltpu.VMEM(padded, jnp.float32), pltpu.VMEM((2,) + padded, jnp.float32)],
        compiler_params=pltpu.CompilerParams(vmem_limit_bytes=SMALL_LIMIT),
        name="sweeps",
    )(faces, both, other)
    return (potential, values)


def solution(mesh):
    return jax.shard_map(
        step_of,
        mesh=mesh,
        in_specs=(P("gx", ("grp", "gy"), None), P("gx", "gy", "grp"), P("gx", "gy", "grp"), P()),
        out_specs=(P("gx", ("grp", "gy"), None), P("gx", "gy", "grp")),
        check_vma=False,
    )
```
